256 devices in a mesh: head: 4 (over z_hi), outer: 4 (over z_lo, core), inner: 16 (over y, x).
Axes of the slice: x: 4, y: 4, z: 8 (z_hi: 4, z_lo: 2; z = z_hi * 2 + z_lo), core: 2. Of those that a mesh axis runs over, the one named last changes fastest.
Arguments:
- query_nope: bfloat16 [8192, 2048], P(('outer', 'inner'), 'head'), may hold values from -6 to 6
- query_rope: bfloat16 [8192, 1024], P(('outer', 'inner'), 'head'), may hold values from -8 to 8
- cache: bfloat16 [8192, 576], P(('outer', 'inner')), may hold values from -8 to 8
- span_ids: int32 [128], P(('outer', 'inner')), may hold values from 0 to 127, as said below
- key_up: bfloat16 [512, 2048], P(None, 'head'), may hold values from -0.25 to 0.25
- value_up: bfloat16 [512, 2048], P(None, 'head'), may hold values from -1.5 to 1.5
- out_proj: bfloat16 [2048, 2048], P('head'), may hold values from -1.1953125 to 1.1953125
Outputs:
- mixed: bfloat16 [8192, 2048], P(('outer', 'inner'), 'head')
The draws below stay inside these ranges and needn't reach their ends.
Inputs may be any that keep to these rules, and one draw needn't show every extreme that they name: `span_ids`: each of 0 to 127 appears once; entries 2 r and 2 r + 1 belong to storage rows r * 128 to (r + 1) * 128 - 1.
All inputs are finite; a program needn't handle non-finite values.
Results may differ from the reference program's by a relative error of at most 0.014.
Values may be sent and summed in bfloat16 or wider, within the bound.
A program may use at most 64 MiB of HBM per device.

```python
import math
import jax
import jax.numpy as jnp
from jax import lax

HEADS = 16
LATENT = 512
ROPE = 64
NOPE = 128
VDIM = 128
MODEL = 2048
SPAN = 64
SPANS = 128
SEQ = 8192


def span_order(key):
    return jax.random.permutation(jax.random.fold_in(key, 7), SPANS).astype(jnp.int32)


def draw_span_ids(key, part):
    return span_order(key)


def draw_cache(key, part):
    values_all = jax.random.normal(jax.random.fold_in(key, 1), (SEQ, LATENT + ROPE), jnp.float32)
    return jnp.clip(values_all, -8.0, 8.0).astype(jnp.bfloat16)


def draw_query_rope(key, part):
    values_all = jax.random.normal(jax.random.fold_in(key, 3), (SEQ, HEADS * ROPE), jnp.float32)
    return jnp.clip(values_all, -8.0, 8.0).astype(jnp.bfloat16)


def block_levels(rng, shape, split, least, high):
    level, own = 1.0, jax.random.fold_in(rng, 6)
    for dim, blocks in split:
        draws = jnp.exp(jax.random.uniform(jax.random.fold_in(own, dim), (blocks,), jnp.float32, least / len(split), high / len(split)))
        level = level * jnp.repeat(draws, shape[dim] // blocks).reshape([-1 if axis == dim else 1 for axis in range(len(shape))])
    return level


def scatter_about(stream_key, shape, width, reach, pieces=(), kind=jnp.bfloat16):
    drawn = width * jax.random.normal(stream_key, shape, jnp.float32)
    if pieces:
        drawn = drawn * block_levels(stream_key, shape, pieces, -0.22, 0.18)
    return jnp.clip(drawn, -reach, reach).astype(kind)


def setup_inputs(seed: int = 0) -> dict:
    key_of = jax.random.split(jax.random.key(seed), 8)
    return {
        "query_nope": scatter_about(key_of[0], (SEQ, HEADS * NOPE), 1.0, 6.0, ((0, 64), (1, 4))),
        "query_rope": draw_query_rope(jax.random.fold_in(key_of[7], 71), 0),
        "cache": draw_cache(jax.random.fold_in(key_of[7], 71), 0),
        "span_ids": draw_span_ids(jax.random.fold_in(key_of[7], 71), 0),
        "key_up": scatter_about(key_of[4], (LATENT, HEADS * NOPE), LATENT ** -0.5, 0.25, ((1, 4),)),
        "value_up": scatter_about(key_of[5], (LATENT, HEADS * VDIM), 0.25, 1.5, ((1, 4),)),
        "out_proj": scatter_about(key_of[6], (HEADS * VDIM, MODEL), 0.2, 1.1953125, ((0, 4),)),
    }


def reference(query_nope, query_rope, cache, span_ids, key_up, value_up, out_proj):
    seq_total = cache.shape[0]
    row_ids = jnp.arange(seq_total, dtype=jnp.int32)
    position = span_ids[row_ids // SPAN] * SPAN + row_ids % SPAN
    query_heads = query_nope.reshape(seq_total, HEADS, NOPE).astype(jnp.float32)
    key_weight = key_up.reshape(LATENT, HEADS, NOPE).astype(jnp.float32)
    q_latent = jnp.einsum("shd,chd->hsc", query_heads, key_weight).astype(jnp.bfloat16)
    q_rotary = jnp.transpose(query_rope.reshape(seq_total, HEADS, ROPE), (1, 0, 2))
    queries = jnp.concatenate([q_latent, q_rotary], axis=2).astype(jnp.float32)
    keys_all = cache.astype(jnp.float32)
    latent_all = keys_all[:, :LATENT]
    value_weight = value_up.reshape(LATENT, HEADS, VDIM).astype(jnp.float32)
    softmax_scale = (NOPE + ROPE) ** -0.5
    block_rows = math.gcd(seq_total, 512)

    def one_block(which_block):
        first_row = which_block * block_rows
        query_block = lax.dynamic_slice_in_dim(queries, first_row, block_rows, 1)
        query_pos = lax.dynamic_slice_in_dim(position, first_row, block_rows, 0)
        scores = jnp.einsum("hsc,tc->hst", query_block, keys_all) * softmax_scale
        visible = position[None, None, :] <= query_pos[None, :, None]
        scores = jnp.where(visible, scores, -jnp.inf)
        row_max = jnp.max(scores, axis=2, keepdims=True)
        expsum = jnp.exp(scores - row_max)
        denom = jnp.sum(expsum, axis=2)
        weights = lax.optimization_barrier(expsum.astype(jnp.bfloat16)).astype(jnp.float32)
        latent_out = jnp.einsum("hst,tc->hsc", weights, latent_all) / denom[:, :, None]
        latent_out = lax.optimization_barrier(latent_out.astype(jnp.bfloat16)).astype(jnp.float32)
        head_out = jnp.einsum("hsc,chd->shd", latent_out, value_weight)
        head_out = head_out.astype(jnp.bfloat16).reshape(block_rows, HEADS * VDIM)
        mixed = jnp.dot(head_out, out_proj, preferred_element_type=jnp.float32)
        return mixed.astype(jnp.bfloat16)

    blocks = lax.map(one_block, jnp.arange(seq_total // block_rows, dtype=jnp.int32))
    return blocks.reshape(seq_total, MODEL)
```

```python
import jax
import jax.numpy as jnp
from jax import lax
from jax.experimental import pallas as pl
from jax.experimental.pallas import tpu as pltpu
from jax.sharding import PartitionSpec as P

LATENT = 512
ROPE = 64
NOPE = 128
SPAN = 64
HEADS_DEV = 4
ROWS = 128
WIDTH = LATENT + ROPE
QWIDTH = HEADS_DEV * (NOPE + ROPE)
R = 4
SUB = ROWS // R
UNIT = HEADS_DEV * 4 * SUB
KROWS = ROWS + 16
HALVES = ((0, 64), (64, 80))
SCALE = (NOPE + ROPE) ** -0.5 * 1.4426950408889634
LOG2E = 1.4426950408889634
LOWEST = -1e30
MESH = pl.DeviceIdType.MESH
TN = (((1,), (1,)), ((), ()))
NN = (((1,), (0,)), ((), ()))
f32 = jnp.float32
bf16 = jnp.bfloat16
CHUNKS = ((0, 4, 8, 12), (1, 3, 5, 7), (2, 6, 9, 11), (10, 13, 14, 15))


def kernel(
    span_ref, qn_ref, qr_ref, k_ref, ku_ref, vu_ref, op_ref, out_ref,
    kbuf, qx, qpos, ku, vu, op, qs, qc, s_sc, m_sc, pbuf, stat, rbuf, rstat,
    ybuf, y1, ysum, y2,
    load_sem, kr_sem, ks_sem, qr_sem, qs_sem, pr_sem, ps_sem, rr_sem, rs_sem, tr_sem, ts_sem,
    zr_sem, zs_sem,
):
    h = lax.axis_index("head")
    o = lax.axis_index("outer")
    i = lax.axis_index("inner")
    zl, c = o // 2, o % 2
    y, x = i // 4, i % 4
    z = h * 2 + zl

    def at_z(zz):
        return (zz // 2, (zz % 2) * 2 + c, i)

    sib = (h, zl * 2 + 1 - c, i)
    yp = (h, o, ((y + 1) % 4) * 4 + x)
    ym = (h, o, ((y + 3) % 4) * 4 + x)
    zp = at_z((z + 1) % 8)
    zm = at_z((z + 7) % 8)
    xs = [None] + [(h, o, y * 4 + (x + d) % 4) for d in (1, 2, 3)]
    hp = ((h + 1) % 4, o, i)
    hm = ((h + 3) % 4, o, i)

    loads = [
        pltpu.make_async_copy(k_ref, kbuf.at[0, pl.ds(0, ROWS)], load_sem.at[0]),
        pltpu.make_async_copy(qn_ref, qx.at[0, :, pl.ds(0, 512)], load_sem.at[1]),
        pltpu.make_async_copy(qr_ref, qx.at[0, :, pl.ds(512, 256)], load_sem.at[2]),
        pltpu.make_async_copy(ku_ref, ku, load_sem.at[3]),
        pltpu.make_async_copy(vu_ref, vu, load_sem.at[4]),
        pltpu.make_async_copy(op_ref, op, load_sem.at[5]),
    ]
    for copy in loads:
        copy.start()
    barrier = pltpu.get_barrier_semaphore()
    for partner in (sib, yp, ym, zp, zm, xs[1], xs[2], xs[3], hp, hm):
        pl.semaphore_signal(barrier, inc=1, device_id=partner, device_id_type=MESH)
    first = span_ref[0].astype(f32)
    second = span_ref[1].astype(f32)
    lane = lax.broadcasted_iota(jnp.int32, (16, 128), 1)
    row = lax.broadcasted_iota(jnp.int32, (16, 128), 0)
    kbuf[0, ROWS:KROWS, :] = jnp.zeros((16, WIDTH), bf16)
    kbuf[0, ROWS:KROWS, 0:128] = jnp.where(lane < SPAN, first, second).astype(bf16)
    qpos[0] = jnp.where(row < 8, first, second).astype(bf16)
    pl.semaphore_wait(barrier, 10)

    sends = []

    def send(src, dst, s_sem, r_sem, device):
        copy = pltpu.make_async_remote_copy(
            src_ref=src, dst_ref=dst, send_sem=s_sem, recv_sem=r_sem,
            device_id=device, device_id_type=MESH,
        )
        copy.start()
        sends.append(copy)

    count = [0]

    def half(slot, b):
        begin, size = HALVES[b]
        return kbuf.at[slot, pl.ds(begin, size)]

    def send_k(slot, b, there, device):
        send(half(slot, b), half(there, b), ks_sem.at[count[0]], kr_sem.at[there, b], device)
        count[0] += 1

    def wait_k(slot, b):
        pltpu.make_async_copy(half(slot, b), half(slot, b), kr_sem.at[slot, b]).wait()

    def qpart(slot, r):
        return qx.at[slot, pl.ds(r * SUB, SUB)]

    def send_q(slot, r, there, device, s_sem):
        send(qpart(slot, r), qpart(there, r), s_sem, qr_sem.at[there, r], device)

    def wait_q(slot, r):
        pltpu.make_async_copy(qpart(slot, r), qpart(slot, r), qr_sem.at[slot, r]).wait()

    loads[0].wait()
    send_k(0, 0, 3, yp)
    send_k(0, 1, 1, ym)
    send_k(0, 0, 8, zp)
    send_k(0, 1, 8, zm)
    send_k(0, 0, 4, sib)
    send_k(0, 1, 4, sib)
    send_k(0, 1, 3, yp)
    send_k(0, 0, 1, ym)
    loads[1].wait()
    loads[2].wait()
    for d in (1, 2, 3):
        send(qpos.at[0], qpos.at[4 - d], ps_sem.at[d - 1], pr_sem.at[4 - d], xs[d])
    for r in range(R):
        send_q(0, r, 3, xs[1], qs_sem.at[0, r])
        send_q(0, r, 1, xs[3], qs_sem.at[1, r])

    def build_q(r):
        rows = pl.ds(r * SUB, SUB)
        for head in range(HEADS_DEV):
            nope = qx[:, rows, head * NOPE : (head + 1) * NOPE].reshape(4 * SUB, NOPE)
            latent = lax.dot_general(
                nope, ku[:, head * NOPE : (head + 1) * NOPE], TN, preferred_element_type=f32
            )
            mine = pl.ds(head * 4 * SUB, 4 * SUB)
            qs[r, mine, 0:LATENT] = latent.astype(bf16)
            begin = HEADS_DEV * NOPE + head * ROPE
            qs[r, mine, LATENT:WIDTH] = qx[:, rows, begin : begin + ROPE].reshape(4 * SUB, ROPE)
        within = lax.broadcasted_iota(jnp.int32, (SUB, 128), 0).astype(f32)
        for d in range(4):
            span = qpos[d].astype(f32)[(r * SUB // SPAN) * 8 : (r * SUB // SPAN) * 8 + 1, :]
            pos = span * SPAN + (within + (r * SUB) % SPAN)
            for head in range(HEADS_DEV):
                qc[r, pl.ds(head * 4 * SUB + d * SUB, SUB), :] = pos
        m_sc[r] = jnp.full((UNIT, 128), LOWEST, f32)

    offset = lax.rem(lax.broadcasted_iota(jnp.int32, (1, 128), 1), SPAN).astype(f32)

    def scores(chunk, r):
        slots = CHUNKS[chunk]
        keys = jnp.concatenate([kbuf[s, 0:ROWS, :] for s in slots], axis=0)
        values = lax.dot_general(qs[r], keys, TN, preferred_element_type=f32)
        rowpos = qc[r]
        peak = m_sc[r]
        for j, s in enumerate(slots):
            keypos = kbuf[s, ROWS:KROWS, 0:128].astype(f32)[0:1, :] * SPAN + offset
            part = jnp.where(
                keypos <= rowpos, values[:, j * 128 : (j + 1) * 128] * SCALE, LOWEST
            )
            s_sc[r, :, s * 128 : (s + 1) * 128] = part
            peak = jnp.maximum(peak, part)
        m_sc[r] = peak

    def scores_for(chunk, low, high):
        def body(r, carry):
            scores(chunk, r)
            return carry

        lax.fori_loop(low, high, body, 0)

    def pass_z(slot):
        send_k(slot, 0, slot + 8, zp)
        send_k(slot, 1, slot + 8, zm)

    wait_k(8, 0)
    send_k(8, 0, 12, sib)
    wait_k(8, 1)
    send_k(8, 1, 12, sib)
    wait_k(3, 0)
    send_k(3, 0, 2, yp)
    send_k(3, 0, 11, zp)
    send_k(3, 0, 7, sib)
    wait_k(1, 1)
    send_k(1, 1, 2, ym)
    send_k(1, 1, 9, zm)
    send_k(1, 1, 5, sib)
    wait_q(3, 0)
    send_q(3, 0, 2, xs[1], qs_sem.at[2, 0])
    wait_k(3, 1)
    send_k(3, 1, 11, zm)
    send_k(3, 1, 7, sib)
    wait_k(1, 0)
    send_k(1, 0, 9, zp)
    send_k(1, 0, 5, sib)
    for d in (1, 2, 3):
        pltpu.make_async_copy(qpos.at[d], qpos.at[d], pr_sem.at[d]).wait()
    loads[3].wait()
    wait_q(1, 0)
    wait_q(2, 0)
    build_q(0)
    for slot in (4, 12):
        for b in (0, 1):
            wait_k(slot, b)
    scores(0, 0)
    wait_q(1, 1)
    send_q(1, 1, 2, xs[3], qs_sem.at[2, 1])
    wait_k(2, 0)
    send_k(2, 0, 10, zp)
    send_k(2, 0, 6, sib)
    wait_k(2, 1)
    send_k(2, 1, 10, zm)
    send_k(2, 1, 6, sib)
    wait_q(3, 1)
    wait_q(2, 1)
    build_q(1)
    scores_for(0, 1, 2)
    for slot in (5, 7):
        for b in (0, 1):
            wait_k(slot, b)
    wait_q(3, 2)
    send_q(3, 2, 2, xs[1], qs_sem.at[2, 2])
    scores_for(1, 0, 2)
    for slot in (11, 9):
        for b in (0, 1):
            wait_k(slot, b)
            send_k(slot, b, slot + 4, sib)
    for b in (0, 1):
        wait_k(6, b)
    wait_q(1, 2)
    wait_q(2, 2)
    build_q(2)
    scores_for(2, 0, 3)
    for b in (0, 1):
        wait_k(10, b)
        send_k(10, b, 14, sib)
    wait_q(1, 3)
    send_q(1, 3, 2, xs[3], qs_sem.at[2, 3])
    scores_for(0, 2, 3)
    scores_for(1, 2, 3)
    for slot in (13, 14, 15):
        for b in (0, 1):
            wait_k(slot, b)
    scores_for(3, 0, 3)
    wait_q(3, 3)
    wait_q(2, 3)
    build_q(3)
    for chunk in range(4):
        scores_for(chunk, 3, 4)
    loads[4].wait()

    def weigh(r):
        top = jnp.max(m_sc[r], axis=1, keepdims=True)
        wide = jnp.broadcast_to(top, (UNIT, 128))
        total = jnp.zeros((UNIT, 128), f32)
        acc = None
        for t in range(4):
            parts = []
            for j in range(4):
                begin = (t * 4 + j) * 128
                w = jnp.exp2(s_sc[r, :, begin : begin + 128] - wide)
                total = total + w
                parts.append(w.astype(bf16))
            latents = jnp.concatenate([kbuf[t * 4 + j, 0:ROWS, 0:LATENT] for j in range(4)], axis=0)
            piece = lax.dot_general(
                jnp.concatenate(parts, axis=1), latents, NN, preferred_element_type=f32
            )
            acc = piece if acc is None else acc + piece
        denom = jnp.sum(total, axis=1, keepdims=True)
        logs = top + jnp.log(denom) * LOG2E
        latent_out = (acc / denom).astype(bf16)
        for head in range(HEADS_DEV):
            mine = slice(head * 4 * SUB, (head + 1) * 4 * SUB)
            part = lax.dot_general(
                latent_out[mine], vu[:, head * 128 : (head + 1) * 128], NN,
                preferred_element_type=f32,
            ).astype(bf16)
            for d in range(4):
                pbuf[r, d, :, head * 128 : (head + 1) * 128] = part[d * SUB : (d + 1) * SUB]
            flat = jnp.transpose(jnp.broadcast_to(logs[mine], (128, 128)))
            stat[r, head : head + 1, :] = flat[0:1, :]
        for d in (1, 3, 2):
            send(pbuf.at[r, d], rbuf.at[r, d - 1], rs_sem.at[r, d - 1], rr_sem.at[r, d - 1], xs[d])
            send(stat.at[r], rstat.at[r, d - 1], ts_sem.at[r, d - 1], tr_sem.at[r, d - 1], xs[d])

    def merge(r):
        for d in (0, 1, 2):
            pltpu.make_async_copy(rbuf.at[r, d], rbuf.at[r, d], rr_sem.at[r, d]).wait()
            pltpu.make_async_copy(rstat.at[r, d], rstat.at[r, d], tr_sem.at[r, d]).wait()
        tiles = [stat[r]] + [rstat[r, d] for d in range(3)]
        columns = [
            jnp.transpose(tile)[d * SUB : (d + 1) * SUB, :] for d, tile in enumerate(tiles)
        ]
        heads = []
        for head in range(HEADS_DEV):
            logs = [col[:, head : head + 1] for col in columns]
            top = jnp.maximum(jnp.maximum(logs[0], logs[1]), jnp.maximum(logs[2], logs[3]))
            scale = [jnp.exp2(v - top) for v in logs]
            total = scale[0] + scale[1] + scale[2] + scale[3]
            where = slice(head * 128, (head + 1) * 128)
            acc = pbuf[r, 0, :, where].astype(f32) * scale[0]
            for d in range(3):
                acc = acc + rbuf[r, d, :, where].astype(f32) * scale[d + 1]
            heads.append((acc / total).astype(bf16))
        head_out = jnp.concatenate(heads, axis=1)
        for d in (2, 1, 3, 0):
            begin = pl.multiple_of(((h + d) % 4) * 512, 512)
            ybuf[r, d] = lax.dot_general(
                head_out, op[:, pl.ds(begin, 512)], NN, preferred_element_type=f32
            ).astype(bf16)
            if d == 2:
                send(
                    ybuf.at[r, 2, :, pl.ds(0, 256)], y1.at[r, 0],
                    zs_sem.at[r, 0], zr_sem.at[r, 0], hp,
                )
                send(
                    ybuf.at[r, 2, :, pl.ds(256, 256)], y1.at[r, 1],
                    zs_sem.at[r, 1], zr_sem.at[r, 1], hm,
                )

    def pass_on(r):
        for b in (0, 1):
            pltpu.make_async_copy(y1.at[r, b], y1.at[r, b], zr_sem.at[r, b]).wait()
        left = ybuf[r, 1, :, 0:256].astype(f32) + y1[r, 0].astype(f32)
        ysum[r, 0, :, 0:256] = left.astype(bf16)
        ysum[r, 0, :, 256:512] = ybuf[r, 1, :, 256:512]
        send(ysum.at[r, 0], y2.at[r, 0], zs_sem.at[r, 2], zr_sem.at[r, 2], hp)
        right = ybuf[r, 3, :, 256:512].astype(f32) + y1[r, 1].astype(f32)
        ysum[r, 1, :, 256:512] = right.astype(bf16)
        ysum[r, 1, :, 0:256] = ybuf[r, 3, :, 0:256]
        send(ysum.at[r, 1], y2.at[r, 1], zs_sem.at[r, 3], zr_sem.at[r, 3], hm)

    def finish(r):
        for b in (0, 1):
            pltpu.make_async_copy(y2.at[r, b], y2.at[r, b], zr_sem.at[r, 2 + b]).wait()
        total = ybuf[r, 0].astype(f32) + y2[r, 0].astype(f32) + y2[r, 1].astype(f32)
        out_ref[r * SUB : (r + 1) * SUB, :] = total.astype(bf16)

    weigh(0)
    weigh(1)
    weigh(2)
    loads[5].wait()
    merge(0)
    weigh(3)
    merge(1)
    pass_on(0)
    merge(2)
    pass_on(1)
    merge(3)
    pass_on(2)
    finish(0)
    pass_on(3)
    finish(1)
    finish(2)
    finish(3)
    for copy in sends:
        copy.wait_send()


def shards(query_nope, query_rope, cache, span_ids, key_up, value_up, out_proj):
    anywhere = pl.BlockSpec(memory_space=pl.ANY)
    dma = pltpu.SemaphoreType.DMA
    return pl.pallas_call(
        kernel,
        name="attend",
        out_shape=jax.ShapeDtypeStruct((ROWS, 512), bf16),
        in_specs=[pl.BlockSpec(memory_space=pltpu.SMEM)] + [anywhere] * 6,
        out_specs=pl.BlockSpec(memory_space=pltpu.VMEM),
        scratch_shapes=[
            pltpu.VMEM((16, KROWS, WIDTH), bf16),
            pltpu.VMEM((4, ROWS, QWIDTH), bf16),
            pltpu.VMEM((4, 16, 128), bf16),
            pltpu.VMEM((512, 512), bf16),
            pltpu.VMEM((512, 512), bf16),
            pltpu.VMEM((512, 2048), bf16),
            pltpu.VMEM((R, UNIT, WIDTH), bf16),
            pltpu.VMEM((R, UNIT, 128), f32),
            pltpu.VMEM((R, UNIT, 2048), f32),
            pltpu.VMEM((R, UNIT, 128), f32),
            pltpu.VMEM((R, 4, SUB, 512), bf16),
            pltpu.VMEM((R, 8, 128), f32),
            pltpu.VMEM((R, 3, SUB, 512), bf16),
            pltpu.VMEM((R, 3, 8, 128), f32),
            pltpu.VMEM((R, 4, SUB, 512), bf16),
            pltpu.VMEM((R, 2, SUB, 256), bf16),
            pltpu.VMEM((R, 2, SUB, 512), bf16),
            pltpu.VMEM((R, 2, SUB, 512), bf16),
            dma((6,)),
            dma((16, 2)),
            dma((40,)),
            dma((4, R)),
            dma((3, R)),
            dma((4,)),
            dma((3,)),
            dma((R, 3)),
            dma((R, 3)),
            dma((R, 3)),
            dma((R, 3)),
            dma((R, 4)),
            dma((R, 4)),
        ],
        compiler_params=pltpu.CompilerParams(
            collective_id=0, has_side_effects=True, vmem_limit_bytes=62 * 2**20
        ),
    )(span_ids, query_nope, query_rope, cache, key_up, value_up, out_proj)


def solution(mesh):
    rows = ("outer", "inner")
    return jax.shard_map(
        shards,
        mesh=mesh,
        in_specs=(
            P(rows, "head"),
            P(rows, "head"),
            P(rows, None),
            P(rows),
            P(None, "head"),
            P(None, "head"),
            P("head", None),
        ),
        out_specs=P(rows, "head"),
        check_vma=False,
    )
```

```python
import jax
import jax.numpy as jnp
from jax import lax
from jax.experimental import pallas as pl
from jax.experimental.pallas import tpu as pltpu
from jax.sharding import PartitionSpec as P

LATENT = 512
ROPE = 64
NOPE = 128
SPAN = 64
HEADS_DEV = 4
ROWS = 128
WIDTH = LATENT + ROPE
QWIDTH = HEADS_DEV * (NOPE + ROPE)
R = 4
SUB = ROWS // R
UNIT = HEADS_DEV * 4 * SUB
KROWS = WIDTH + 16
HALVES = ((0, 288), (288, 304))
SCALE = (NOPE + ROPE) ** -0.5 * 1.4426950408889634
LOG2E = 1.4426950408889634
LOWEST = -1e30
MESH = pl.DeviceIdType.MESH
TN = (((1,), (1,)), ((), ()))
NN = (((1,), (0,)), ((), ()))
f32 = jnp.float32
bf16 = jnp.bfloat16
CHUNKS = ((0, 4, 8, 12), (1, 3, 5, 7), (2, 6, 9, 11), (10, 13, 14, 15))


def kernel(
    span_ref, qn_ref, qr_ref, k_ref, ku_ref, vu_ref, op_ref, out_ref,
    kbuf, qx, qpos, ku, vu, op, qs, qc, s_sc, m_sc, pbuf, stat, rbuf, rstat,
    ybuf, y1, ysum, y2,
    load_sem, kr_sem, ks_sem, qr_sem, qs_sem, pr_sem, ps_sem, rr_sem, rs_sem, tr_sem, ts_sem,
    zr_sem, zs_sem,
):
    h = lax.axis_index("head")
    o = lax.axis_index("outer")
    i = lax.axis_index("inner")
    zl, c = o // 2, o % 2
    y, x = i // 4, i % 4
    z = h * 2 + zl

    def at_z(zz):
        return (zz // 2, (zz % 2) * 2 + c, i)

    sib = (h, zl * 2 + 1 - c, i)
    yp = (h, o, ((y + 1) % 4) * 4 + x)
    ym = (h, o, ((y + 3) % 4) * 4 + x)
    zp = at_z((z + 1) % 8)
    zm = at_z((z + 7) % 8)
    xs = [None] + [(h, o, y * 4 + (x + d) % 4) for d in (1, 2, 3)]
    hp = ((h + 1) % 4, o, i)
    hm = ((h + 3) % 4, o, i)

    loads = [
        pltpu.make_async_copy(k_ref, kbuf.at[0, pl.ds(0, WIDTH)], load_sem.at[0]),
        pltpu.make_async_copy(qn_ref, qx.at[0, :, pl.ds(0, 512)], load_sem.at[1]),
        pltpu.make_async_copy(qr_ref, qx.at[0, :, pl.ds(512, 256)], load_sem.at[2]),
        pltpu.make_async_copy(ku_ref, ku, load_sem.at[3]),
        pltpu.make_async_copy(vu_ref, vu, load_sem.at[4]),
        pltpu.make_async_copy(op_ref, op, load_sem.at[5]),
    ]
    barrier = pltpu.get_barrier_semaphore()
    near = (sib, yp, ym, zp, zm, xs[1], xs[3])
    for partner in near:
        pl.semaphore_signal(barrier, inc=1, device_id=partner, device_id_type=MESH)
    for copy in loads:
        copy.start()
    first = span_ref[0].astype(f32)
    second = span_ref[1].astype(f32)
    lane = lax.broadcasted_iota(jnp.int32, (16, 128), 1)
    row = lax.broadcasted_iota(jnp.int32, (16, 128), 0)
    kbuf[0, WIDTH:KROWS, :] = jnp.where(lane < SPAN, first, second).astype(bf16)
    qpos[0] = jnp.where(row < 8, first, second).astype(bf16)
    loads[0].wait()
    pl.semaphore_wait(barrier, len(near))

    sends = []

    def send(src, dst, s_sem, r_sem, device):
        copy = pltpu.make_async_remote_copy(
            src_ref=src, dst_ref=dst, send_sem=s_sem, recv_sem=r_sem,
            device_id=device, device_id_type=MESH,
        )
        copy.start()
        sends.append(copy)

    count = [0, 0]

    def half(slot, b):
        begin, size = HALVES[b]
        return kbuf.at[slot, pl.ds(begin, size)]

    def send_k(slot, b, there, device):
        send(half(slot, b), half(there, b), ks_sem.at[count[0]], kr_sem.at[there, b], device)
        count[0] += 1

    def wait_k(slot, b):
        pltpu.make_async_copy(half(slot, b), half(slot, b), kr_sem.at[slot, b]).wait()

    def qpart(slot, b):
        return qx.at[slot, pl.ds(b * SPAN, SPAN)]

    def send_q(slot, b, there, device):
        send(qpart(slot, b), qpart(there, b), qs_sem.at[count[1]], qr_sem.at[there, b], device)
        count[1] += 1

    def wait_q(slot, b):
        pltpu.make_async_copy(qpart(slot, b), qpart(slot, b), qr_sem.at[slot, b]).wait()

    def send_pos(slot, there, device, n):
        send(qpos.at[slot], qpos.at[there], ps_sem.at[n], pr_sem.at[there], device)

    def wait_pos(slot):
        pltpu.make_async_copy(qpos.at[slot], qpos.at[slot], pr_sem.at[slot]).wait()

    send_k(0, 0, 3, yp)
    send_k(0, 1, 1, ym)
    send_k(0, 0, 8, zp)
    send_k(0, 1, 8, zm)
    send_k(0, 0, 4, sib)
    send_k(0, 1, 4, sib)
    send_pos(0, 3, xs[1], 0)
    send_pos(0, 1, xs[3], 1)
    loads[1].wait()
    loads[2].wait()
    send_q(0, 0, 3, xs[1])
    send_q(0, 1, 1, xs[3])
    send_k(0, 1, 3, yp)
    send_k(0, 0, 1, ym)
    send_q(0, 1, 3, xs[1])
    send_q(0, 0, 1, xs[3])

    within = lax.rem(lax.broadcasted_iota(jnp.int32, (ROWS, 128), 0), SPAN).astype(f32)

    def build_q(d):
        for head in range(HEADS_DEV):
            latent = lax.dot_general(
                qx[d, :, head * NOPE : (head + 1) * NOPE],
                ku[:, head * NOPE : (head + 1) * NOPE], TN, preferred_element_type=f32,
            )
            mine = slice(head * ROWS, (head + 1) * ROWS)
            qs[d, mine, 0:LATENT] = latent.astype(bf16)
            begin = HEADS_DEV * NOPE + head * ROPE
            qs[d, mine, LATENT:WIDTH] = qx[d, :, begin : begin + ROPE]
        spans = qpos[d].astype(f32)
        span = jnp.concatenate(
            [jnp.broadcast_to(spans[v : v + 1, :], (SPAN, 128)) for v in (0, 8)], axis=0
        )
        qc[d] = span * SPAN + within

    offset = lax.rem(lax.broadcasted_iota(jnp.int32, (1, 128), 1), SPAN).astype(f32)
    seen = set()

    def scores(chunk, d):
        slots = CHUNKS[chunk]
        keys = jnp.concatenate([kbuf[s, 0:WIDTH, :] for s in slots], axis=1)
        values = lax.dot_general(qs[d], keys, NN, preferred_element_type=f32)
        for head in range(HEADS_DEV):
            rowpos = qc[d]
            peak = m_sc[d, head] if d in seen else None
            for j, s in enumerate(slots):
                keypos = kbuf[s, WIDTH:KROWS, :].astype(f32)[0:1, :] * SPAN + offset
                part = values[head * ROWS : (head + 1) * ROWS, j * 128 : (j + 1) * 128]
                part = jnp.where(keypos <= rowpos, part * SCALE, LOWEST)
                s_sc[d, head, :, s * 128 : (s + 1) * 128] = part
                peak = part if peak is None else jnp.maximum(peak, part)
            m_sc[d, head] = peak
        seen.add(d)

    loads[3].wait()
    build_q(0)
    for b in (0, 1):
        wait_k(8, b)
        send_k(8, b, 12, sib)
    wait_k(3, 0)
    send_k(3, 0, 2, yp)
    send_k(3, 0, 11, zp)
    send_k(3, 0, 7, sib)
    wait_k(1, 1)
    send_k(1, 1, 2, ym)
    send_k(1, 1, 9, zm)
    send_k(1, 1, 5, sib)
    wait_q(3, 0)
    send_q(3, 0, 2, xs[1])
    wait_q(1, 1)
    send_q(1, 1, 2, xs[3])
    wait_pos(3)
    send_pos(3, 2, xs[1], 2)
    wait_pos(1)
    for slot in (4, 12):
        for b in (0, 1):
            wait_k(slot, b)
    scores(0, 0)
    wait_k(3, 1)
    send_k(3, 1, 11, zm)
    send_k(3, 1, 7, sib)
    wait_k(1, 0)
    send_k(1, 0, 9, zp)
    send_k(1, 0, 5, sib)
    wait_q(3, 1)
    build_q(3)
    wait_q(1, 0)
    build_q(1)
    wait_k(2, 0)
    send_k(2, 0, 10, zp)
    send_k(2, 0, 6, sib)
    wait_k(2, 1)
    send_k(2, 1, 10, zm)
    send_k(2, 1, 6, sib)
    for slot in (5, 7):
        for b in (0, 1):
            wait_k(slot, b)
    scores(1, 0)
    scores(0, 3)
    scores(0, 1)
    for slot, b in ((11, 0), (9, 1), (11, 1), (9, 0)):
        wait_k(slot, b)
        send_k(slot, b, slot + 4, sib)
    scores(1, 3)
    scores(1, 1)
    for b in (0, 1):
        wait_k(10, b)
        send_k(10, b, 14, sib)
    for b in (0, 1):
        wait_q(2, b)
    wait_pos(2)
    build_q(2)
    scores(0, 2)
    scores(1, 2)
    for b in (0, 1):
        wait_k(6, b)
    for d in (0, 3, 1, 2):
        scores(2, d)
    for slot in (13, 15, 14):
        for b in (0, 1):
            wait_k(slot, b)
    for d in (0, 3, 1, 2):
        scores(3, d)
    loads[4].wait()

    def weigh(r):
        rows = slice(r * SUB, (r + 1) * SUB)
        top = jnp.max(m_sc[:, :, rows, :].reshape(UNIT, 128), axis=1, keepdims=True)
        wide = jnp.broadcast_to(top, (UNIT, 128))
        total = jnp.zeros((UNIT, 128), f32)
        acc = None
        for t in range(4):
            parts = []
            for j in range(4):
                begin = (t * 4 + j) * 128
                w = jnp.exp2(s_sc[:, :, rows, begin : begin + 128].reshape(UNIT, 128) - wide)
                total = total + w
                parts.append(w.astype(bf16))
            latents = jnp.concatenate([kbuf[t * 4 + j, 0:LATENT, :] for j in range(4)], axis=1)
            piece = lax.dot_general(
                jnp.concatenate(parts, axis=1), latents, TN, preferred_element_type=f32
            )
            acc = piece if acc is None else acc + piece
        denom = jnp.sum(total, axis=1, keepdims=True)
        logs = (top + jnp.log(denom) * LOG2E).reshape(4, HEADS_DEV, SUB, 1)
        latent_out = (acc / denom).astype(bf16).reshape(4, HEADS_DEV, SUB, LATENT)
        for head in range(HEADS_DEV):
            part = lax.dot_general(
                latent_out[:, head].reshape(4 * SUB, LATENT),
                vu[:, head * 128 : (head + 1) * 128], NN, preferred_element_type=f32,
            ).astype(bf16)
            for d in range(4):
                pbuf[r, d, :, head * 128 : (head + 1) * 128] = part[d * SUB : (d + 1) * SUB]
            flat = jnp.transpose(jnp.broadcast_to(logs[:, head].reshape(4 * SUB, 1), (128, 128)))
            stat[r, head : head + 1, :] = flat[0:1, :]
        for d in (2, 1, 3):
            send(pbuf.at[r, d], rbuf.at[r, d - 1], rs_sem.at[r, d - 1], rr_sem.at[r, d - 1], xs[d])
            send(stat.at[r], rstat.at[r, d - 1], ts_sem.at[r, d - 1], tr_sem.at[r, d - 1], xs[d])

    def merge(r):
        for d in (0, 1, 2):
            pltpu.make_async_copy(rbuf.at[r, d], rbuf.at[r, d], rr_sem.at[r, d]).wait()
            pltpu.make_async_copy(rstat.at[r, d], rstat.at[r, d], tr_sem.at[r, d]).wait()
        tiles = [stat[r]] + [rstat[r, d] for d in range(3)]
        columns = [
            jnp.transpose(tile)[d * SUB : (d + 1) * SUB, :] for d, tile in enumerate(tiles)
        ]
        heads = []
        for head in range(HEADS_DEV):
            logs = [col[:, head : head + 1] for col in columns]
            top = jnp.maximum(jnp.maximum(logs[0], logs[1]), jnp.maximum(logs[2], logs[3]))
            scale = [jnp.exp2(v - top) for v in logs]
            total = scale[0] + scale[1] + scale[2] + scale[3]
            where = slice(head * 128, (head + 1) * 128)
            acc = pbuf[r, 0, :, where].astype(f32) * scale[0]
            for d in range(3):
                acc = acc + rbuf[r, d, :, where].astype(f32) * scale[d + 1]
            heads.append((acc / total).astype(bf16))
        head_out = jnp.concatenate(heads, axis=1)
        for d in (2, 1, 3, 0):
            begin = pl.multiple_of(((h + d) % 4) * 512, 512)
            ybuf[r, d] = lax.dot_general(
                head_out, op[:, pl.ds(begin, 512)], NN, preferred_element_type=f32
            ).astype(bf16)
            if d == 2:
                send(
                    ybuf.at[r, 2, :, pl.ds(0, 256)], y1.at[r, 0],
                    zs_sem.at[r, 0], zr_sem.at[r, 0], hp,
                )
                send(
                    ybuf.at[r, 2, :, pl.ds(256, 256)], y1.at[r, 1],
                    zs_sem.at[r, 1], zr_sem.at[r, 1], hm,
                )

    def pass_on(r):
        for b in (0, 1):
            pltpu.make_async_copy(y1.at[r, b], y1.at[r, b], zr_sem.at[r, b]).wait()
        left = ybuf[r, 1, :, 0:256].astype(f32) + y1[r, 0].astype(f32)
        ysum[r, 0, :, 0:256] = left.astype(bf16)
        ysum[r, 0, :, 256:512] = ybuf[r, 1, :, 256:512]
        send(ysum.at[r, 0], y2.at[r, 0], zs_sem.at[r, 2], zr_sem.at[r, 2], hp)
        right = ybuf[r, 3, :, 256:512].astype(f32) + y1[r, 1].astype(f32)
        ysum[r, 1, :, 256:512] = right.astype(bf16)
        ysum[r, 1, :, 0:256] = ybuf[r, 3, :, 0:256]
        send(ysum.at[r, 1], y2.at[r, 1], zs_sem.at[r, 3], zr_sem.at[r, 3], hm)

    def finish(r):
        for b in (0, 1):
            pltpu.make_async_copy(y2.at[r, b], y2.at[r, b], zr_sem.at[r, 2 + b]).wait()
        total = ybuf[r, 0].astype(f32) + y2[r, 0].astype(f32) + y2[r, 1].astype(f32)
        out_ref[r * SUB : (r + 1) * SUB, :] = total.astype(bf16)

    weigh(0)
    weigh(1)
    weigh(2)
    loads[5].wait()
    merge(0)
    weigh(3)
    merge(1)
    pass_on(0)
    merge(2)
    pass_on(1)
    merge(3)
    pass_on(2)
    finish(0)
    pass_on(3)
    finish(1)
    finish(2)
    finish(3)
    for copy in sends:
        copy.wait_send()


def shards(query_nope, query_rope, cache, span_ids, key_up, value_up, out_proj):
    anywhere = pl.BlockSpec(memory_space=pl.ANY)
    dma = pltpu.SemaphoreType.DMA
    return pl.pallas_call(
        kernel,
        name="attend",
        out_shape=jax.ShapeDtypeStruct((ROWS, 512), bf16),
        in_specs=[pl.BlockSpec(memory_space=pltpu.SMEM)] + [anywhere] * 6,
        out_specs=pl.BlockSpec(memory_space=pltpu.VMEM),
        scratch_shapes=[
            pltpu.VMEM((16, KROWS, ROWS), bf16),
            pltpu.VMEM((4, ROWS, QWIDTH), bf16),
            pltpu.VMEM((4, 16, 128), bf16),
            pltpu.VMEM((512, 512), bf16),
            pltpu.VMEM((512, 512), bf16),
            pltpu.VMEM((512, 2048), bf16),
            pltpu.VMEM((4, HEADS_DEV * ROWS, WIDTH), bf16),
            pltpu.VMEM((4, ROWS, 128), f32),
            pltpu.VMEM((4, HEADS_DEV, ROWS, 16 * ROWS), f32),
            pltpu.VMEM((4, HEADS_DEV, ROWS, 128), f32),
            pltpu.VMEM((R, 4, SUB, 512), bf16),
            pltpu.VMEM((R, 8, 128), f32),
            pltpu.VMEM((R, 3, SUB, 512), bf16),
            pltpu.VMEM((R, 3, 8, 128), f32),
            pltpu.VMEM((R, 4, SUB, 512), bf16),
            pltpu.VMEM((R, 2, SUB, 256), bf16),
            pltpu.VMEM((R, 2, SUB, 512), bf16),
            pltpu.VMEM((R, 2, SUB, 512), bf16),
            dma((6,)),
            dma((16, 2)),
            dma((40,)),
            dma((4, 2)),
            dma((6,)),
            dma((4,)),
            dma((3,)),
            dma((R, 3)),
            dma((R, 3)),
            dma((R, 3)),
            dma((R, 3)),
            dma((R, 4)),
            dma((R, 4)),
        ],
        compiler_params=pltpu.CompilerParams(
            collective_id=0, has_side_effects=True, vmem_limit_bytes=62 * 2**20
        ),
    )(span_ids, query_nope, query_rope, cache.T, key_up, value_up, out_proj)


def solution(mesh):
    rows = ("outer", "inner")
    return jax.shard_map(
        shards,
        mesh=mesh,
        in_specs=(
            P(rows, "head"),
            P(rows, "head"),
            P(rows, None),
            P(rows),
            P(None, "head"),
            P(None, "head"),
            P("head", None),
        ),
        out_specs=P(rows, "head"),
        check_vma=False,
    )
```

```python
import jax
import jax.numpy as jnp
from jax import lax
from jax.experimental import pallas as pl
from jax.experimental.pallas import tpu as pltpu
from jax.sharding import PartitionSpec as P

LATENT = 512
ROPE = 64
NOPE = 128
SPAN = 64
HEADS_DEV = 4
ROWS = 128
WIDTH = LATENT + ROPE
QWIDTH = HEADS_DEV * (NOPE + ROPE)
R = 4
SUB = ROWS // R
UNIT = HEADS_DEV * 4 * SUB
KROWS = WIDTH + 16
HALVES = ((0, 288), (288, 304))
SCALE = (NOPE + ROPE) ** -0.5 * 1.4426950408889634
LOG2E = 1.4426950408889634
LOWEST = -1e30
MESH = pl.DeviceIdType.MESH
TN = (((1,), (1,)), ((), ()))
NN = (((1,), (0,)), ((), ()))
f32 = jnp.float32
bf16 = jnp.bfloat16
BOTH = (4, 5, 6, 7, 12, 13, 14, 15)
KEY_SEM = {}
for _slot in range(1, 16):
    for _b in (0, 1):
        if _slot in BOTH and _b == 1:
            KEY_SEM[_slot, 1] = KEY_SEM[_slot, 0]
        else:
            KEY_SEM[_slot, _b] = len(set(KEY_SEM.values()))
CHUNKS = ((0, 4, 8, 12), (1, 3, 5, 7), (2, 6, 9, 11), (10, 13, 14, 15))


def kernel(
    span_ref, qn_ref, qr_ref, k_ref, ku_ref, vu_ref, op_ref, out_ref,
    kbuf, qx, qpos, ku, vu, op, qs, qc, s_sc, m_sc, pbuf, stat, rbuf, rstat,
    ybuf, y1, ysum, y2,
    load_sem, kr_sem, qr_sem, pr_sem, rr_sem, tr_sem, zr_sem, send_sem,
):
    h = lax.axis_index("head")
    o = lax.axis_index("outer")
    i = lax.axis_index("inner")
    zl, c = o // 2, o % 2
    y, x = i // 4, i % 4
    z = h * 2 + zl

    def at_z(zz):
        return (zz // 2, (zz % 2) * 2 + c, i)

    sib = (h, zl * 2 + 1 - c, i)
    yp = (h, o, ((y + 1) % 4) * 4 + x)
    ym = (h, o, ((y + 3) % 4) * 4 + x)
    zp = at_z((z + 1) % 8)
    zm = at_z((z + 7) % 8)
    xs = [None] + [(h, o, y * 4 + (x + d) % 4) for d in (1, 2, 3)]
    hp = ((h + 1) % 4, o, i)
    hm = ((h + 3) % 4, o, i)

    loads = [
        pltpu.make_async_copy(k_ref, kbuf.at[0, pl.ds(0, WIDTH)], load_sem.at[0]),
        pltpu.make_async_copy(qn_ref, qx.at[0, :, pl.ds(0, 512)], load_sem.at[1]),
        pltpu.make_async_copy(qr_ref, qx.at[0, :, pl.ds(512, 256)], load_sem.at[2]),
        pltpu.make_async_copy(ku_ref, ku, load_sem.at[3]),
        pltpu.make_async_copy(vu_ref, vu, load_sem.at[4]),
        pltpu.make_async_copy(op_ref, op, load_sem.at[5]),
    ]
    barrier = pltpu.get_barrier_semaphore()
    near = (sib, yp, ym, zp, zm, xs[1], xs[3])
    for partner in near:
        pl.semaphore_signal(barrier, inc=1, device_id=partner, device_id_type=MESH)
    for copy in loads:
        copy.start()
    first = span_ref[0].astype(f32)
    second = span_ref[1].astype(f32)
    lane = lax.broadcasted_iota(jnp.int32, (16, 128), 1)
    row = lax.broadcasted_iota(jnp.int32, (16, 128), 0)
    kbuf[0, WIDTH:KROWS, :] = jnp.where(lane < SPAN, first, second).astype(bf16)
    qpos[0] = jnp.where(row < 8, first, second).astype(bf16)
    loads[0].wait()
    pl.semaphore_wait(barrier, len(near))

    def send(src, dst, kind, r_sem, device):
        pltpu.make_async_remote_copy(
            src_ref=src, dst_ref=dst, send_sem=send_sem.at[kind], recv_sem=r_sem,
            device_id=device, device_id_type=MESH,
        ).start()

    def arrived(ref, sem):
        pltpu.make_async_copy(ref, ref, sem).wait()

    def half(slot, b):
        begin, size = HALVES[b]
        return kbuf.at[slot, pl.ds(begin, size)]

    def send_k(slot, b, there, device):
        send(half(slot, b), half(there, b), 0, kr_sem.at[KEY_SEM[there, b]], device)

    def wait_k(slot, b=None):
        if slot in BOTH:
            arrived(kbuf.at[slot], kr_sem.at[KEY_SEM[slot, 0]])
        else:
            arrived(half(slot, b), kr_sem.at[KEY_SEM[slot, b]])

    def qpart(slot, b):
        return qx.at[slot, pl.ds(b * SPAN, SPAN)]

    def send_q(slot, b, there, device):
        send(qpart(slot, b), qpart(there, b), 1, qr_sem.at[there - 1, b], device)

    def wait_q(slot, b):
        arrived(qpart(slot, b), qr_sem.at[slot - 1, b])

    def send_pos(slot, there, device):
        send(qpos.at[slot], qpos.at[there], 2, pr_sem.at[there - 1], device)

    def wait_pos(slot):
        arrived(qpos.at[slot], pr_sem.at[slot - 1])

    send_k(0, 0, 3, yp)
    send_k(0, 1, 1, ym)
    send_k(0, 0, 8, zp)
    send_k(0, 1, 8, zm)
    send_k(0, 0, 4, sib)
    send_k(0, 1, 4, sib)
    send_pos(0, 3, xs[1])
    send_pos(0, 1, xs[3])
    loads[1].wait()
    loads[2].wait()
    send_q(0, 0, 3, xs[1])
    send_q(0, 1, 1, xs[3])
    send_k(0, 1, 3, yp)
    send_k(0, 0, 1, ym)
    send_q(0, 1, 3, xs[1])
    send_q(0, 0, 1, xs[3])

    within = lax.rem(lax.broadcasted_iota(jnp.int32, (ROWS, 128), 0), SPAN).astype(f32)

    def build_q(d):
        for head in range(HEADS_DEV):
            latent = lax.dot_general(
                qx[d, :, head * NOPE : (head + 1) * NOPE],
                ku[:, head * NOPE : (head + 1) * NOPE], TN, preferred_element_type=f32,
            )
            mine = slice(head * ROWS, (head + 1) * ROWS)
            qs[d, mine, 0:LATENT] = latent.astype(bf16)
            begin = HEADS_DEV * NOPE + head * ROPE
            qs[d, mine, LATENT:WIDTH] = qx[d, :, begin : begin + ROPE]
        spans = qpos[d].astype(f32)
        span = jnp.concatenate(
            [jnp.broadcast_to(spans[v : v + 1, :], (SPAN, 128)) for v in (0, 8)], axis=0
        )
        qc[d] = span * SPAN + within

    offset = lax.rem(lax.broadcasted_iota(jnp.int32, (1, 128), 1), SPAN).astype(f32)
    seen = set()

    def scores(chunk, sources):
        slots = CHUNKS[chunk]
        keys = jnp.concatenate([kbuf[s, 0:WIDTH, :] for s in slots], axis=1)
        queries = jnp.concatenate([qs[d] for d in sources], axis=0)
        values = lax.dot_general(queries, keys, NN, preferred_element_type=f32)
        for n, d in enumerate(sources):
            rowpos = qc[d]
            for head in range(HEADS_DEV):
                begin = (n * HEADS_DEV + head) * ROWS
                peak = m_sc[d, head] if d in seen else None
                for j, s in enumerate(slots):
                    keypos = kbuf[s, WIDTH:KROWS, :].astype(f32)[0:1, :] * SPAN + offset
                    part = values[begin : begin + ROWS, j * 128 : (j + 1) * 128]
                    part = jnp.where(keypos <= rowpos, part * SCALE, LOWEST)
                    s_sc[d, head, :, s * 128 : (s + 1) * 128] = part
                    peak = part if peak is None else jnp.maximum(peak, part)
                m_sc[d, head] = peak
            seen.add(d)

    loads[3].wait()
    build_q(0)
    wait_k(3, 0)
    send_k(3, 0, 2, yp)
    send_k(3, 0, 11, zp)
    send_k(3, 0, 7, sib)
    wait_k(1, 1)
    send_k(1, 1, 2, ym)
    send_k(1, 1, 9, zm)
    send_k(1, 1, 5, sib)
    wait_q(3, 0)
    send_q(3, 0, 2, xs[1])
    wait_q(1, 1)
    send_q(1, 1, 2, xs[3])
    wait_pos(3)
    send_pos(3, 2, xs[1])
    wait_pos(1)
    for b in (0, 1):
        wait_k(8, b)
        send_k(8, b, 12, sib)
    wait_k(3, 1)
    send_k(3, 1, 11, zm)
    send_k(3, 1, 7, sib)
    wait_k(1, 0)
    send_k(1, 0, 9, zp)
    send_k(1, 0, 5, sib)
    wait_k(4)
    wait_k(12)
    scores(0, (0,))
    wait_q(3, 1)
    build_q(3)
    wait_q(1, 0)
    build_q(1)
    wait_k(2, 0)
    send_k(2, 0, 10, zp)
    send_k(2, 0, 6, sib)
    wait_k(2, 1)
    send_k(2, 1, 10, zm)
    send_k(2, 1, 6, sib)
    scores(0, (3, 1))
    for slot, b in ((11, 0), (9, 1), (11, 1), (9, 0)):
        wait_k(slot, b)
        send_k(slot, b, slot + 4, sib)
    wait_k(5)
    wait_k(7)
    scores(1, (0,))
    scores(1, (3, 1))
    for b in (0, 1):
        wait_k(10, b)
        send_k(10, b, 14, sib)
    for b in (0, 1):
        wait_q(2, b)
    wait_pos(2)
    build_q(2)
    scores(0, (2,))
    scores(1, (2,))
    wait_k(6)
    scores(2, (0, 3))
    scores(2, (1, 2))
    wait_k(13)
    wait_k(15)
    wait_k(14)
    loads[4].wait()

    def weigh(r):
        rows = slice(r * SUB, (r + 1) * SUB)
        slots = CHUNKS[3]
        pairs = [(d, head) for d in range(4) for head in range(HEADS_DEV)]
        queries = jnp.concatenate(
            [qs[d, head * ROWS + r * SUB : head * ROWS + (r + 1) * SUB, :] for d, head in pairs],
            axis=0,
        )
        keys = jnp.concatenate([kbuf[s, 0:WIDTH, :] for s in slots], axis=1)
        values = lax.dot_general(queries, keys, NN, preferred_element_type=f32)
        peaks = []
        for n, (d, head) in enumerate(pairs):
            rowpos = qc[d, rows, :]
            peak = m_sc[d, head, rows, :]
            for j, s in enumerate(slots):
                keypos = kbuf[s, WIDTH:KROWS, :].astype(f32)[0:1, :] * SPAN + offset
                part = values[n * SUB : (n + 1) * SUB, j * 128 : (j + 1) * 128]
                part = jnp.where(keypos <= rowpos, part * SCALE, LOWEST)
                s_sc[d, head, rows, s * 128 : (s + 1) * 128] = part
                peak = jnp.maximum(peak, part)
            peaks.append(peak)
        top = jnp.max(jnp.concatenate(peaks, axis=0), axis=1, keepdims=True)
        wide = jnp.broadcast_to(top, (UNIT, 128))
        total = jnp.zeros((UNIT, 128), f32)
        acc = None
        for t in range(4):
            parts = []
            for j in range(4):
                begin = (t * 4 + j) * 128
                w = jnp.exp2(s_sc[:, :, rows, begin : begin + 128].reshape(UNIT, 128) - wide)
                total = total + w
                parts.append(w.astype(bf16))
            latents = jnp.concatenate([kbuf[t * 4 + j, 0:LATENT, :] for j in range(4)], axis=1)
            piece = lax.dot_general(
                jnp.concatenate(parts, axis=1), latents, TN, preferred_element_type=f32
            )
            acc = piece if acc is None else acc + piece
        denom = jnp.sum(total, axis=1, keepdims=True)
        logs = (top + jnp.log(denom) * LOG2E).reshape(4, HEADS_DEV, SUB, 1)
        latent_out = (acc * (1.0 / denom)).astype(bf16).reshape(4, HEADS_DEV, SUB, LATENT)
        outs = [
            lax.dot_general(
                latent_out[:, head].reshape(4 * SUB, LATENT),
                vu[:, head * 128 : (head + 1) * 128], NN, preferred_element_type=f32,
            ).astype(bf16)
            for head in range(HEADS_DEV)
        ]
        for head in range(HEADS_DEV):
            for d in range(4):
                pbuf[r, d, :, head * 128 : (head + 1) * 128] = outs[head][d * SUB : (d + 1) * SUB]
            flat = jnp.transpose(jnp.broadcast_to(logs[:, head].reshape(4 * SUB, 1), (128, 128)))
            stat[r, head : head + 1, :] = flat[0:1, :]
        for d in (2, 1, 3):
            send(pbuf.at[r, d], rbuf.at[r, d - 1], 3, rr_sem.at[r], xs[d])
            send(stat.at[r], rstat.at[r, d - 1], 4, tr_sem.at[r], xs[d])

    def merge(r):
        arrived(rstat.at[r], tr_sem.at[r])
        arrived(rbuf.at[r], rr_sem.at[r])
        tiles = [stat[r]] + [rstat[r, d] for d in range(3)]
        columns = [
            jnp.transpose(tile)[d * SUB : (d + 1) * SUB, :] for d, tile in enumerate(tiles)
        ]
        heads = []
        for head in range(HEADS_DEV):
            logs = [col[:, head : head + 1] for col in columns]
            top = jnp.maximum(jnp.maximum(logs[0], logs[1]), jnp.maximum(logs[2], logs[3]))
            scale = [jnp.exp2(v - top) for v in logs]
            total = scale[0] + scale[1] + scale[2] + scale[3]
            where = slice(head * 128, (head + 1) * 128)
            acc = pbuf[r, 0, :, where].astype(f32) * scale[0]
            for d in range(3):
                acc = acc + rbuf[r, d, :, where].astype(f32) * scale[d + 1]
            heads.append((acc / total).astype(bf16))
        head_out = jnp.concatenate(heads, axis=1)
        for d in (2, 1, 3, 0):
            begin = pl.multiple_of(((h + d) % 4) * 512, 512)
            ybuf[r, d] = lax.dot_general(
                head_out, op[:, pl.ds(begin, 512)], NN, preferred_element_type=f32
            ).astype(bf16)
            if d == 2:
                send(
                    ybuf.at[r, 2, :, pl.ds(0, 256)], y1.at[r, 0], 5, zr_sem.at[r, 0], hp,
                )
                send(
                    ybuf.at[r, 2, :, pl.ds(256, 256)], y1.at[r, 1], 5, zr_sem.at[r, 1], hm,
                )

    def pass_on(r):
        arrived(y1.at[r, 0], zr_sem.at[r, 0])
        left = ybuf[r, 1, :, 0:256].astype(f32) + y1[r, 0].astype(f32)
        ysum[r, 0, :, 0:256] = left.astype(bf16)
        ysum[r, 0, :, 256:512] = ybuf[r, 1, :, 256:512]
        send(ysum.at[r, 0], y2.at[r, 0], 6, zr_sem.at[r, 2], hp)
        arrived(y1.at[r, 1], zr_sem.at[r, 1])
        right = ybuf[r, 3, :, 256:512].astype(f32) + y1[r, 1].astype(f32)
        ysum[r, 1, :, 256:512] = right.astype(bf16)
        ysum[r, 1, :, 0:256] = ybuf[r, 3, :, 0:256]
        send(ysum.at[r, 1], y2.at[r, 1], 6, zr_sem.at[r, 2], hm)

    def finish(r):
        arrived(y2.at[r], zr_sem.at[r, 2])
        total = ybuf[r, 0].astype(f32) + y2[r, 0].astype(f32) + y2[r, 1].astype(f32)
        out_ref[r * SUB : (r + 1) * SUB, :] = total.astype(bf16)

    weigh(0)
    weigh(1)
    weigh(2)
    loads[5].wait()
    merge(0)
    weigh(3)
    merge(1)
    pass_on(0)
    merge(2)
    pass_on(1)
    merge(3)
    pass_on(2)
    finish(0)
    pass_on(3)
    finish(1)
    finish(2)
    finish(3)
    for kind, ref in enumerate((
        kbuf.at[pl.ds(0, 15)], qx.at[pl.ds(0, 3)], qpos.at[pl.ds(0, 3)], rbuf, rstat, y1, y2,
    )):
        arrived(ref, send_sem.at[kind])


def shards(query_nope, query_rope, cache, span_ids, key_up, value_up, out_proj):
    anywhere = pl.BlockSpec(memory_space=pl.ANY)
    dma = pltpu.SemaphoreType.DMA
    return pl.pallas_call(
        kernel,
        name="attend",
        out_shape=jax.ShapeDtypeStruct((ROWS, 512), bf16),
        in_specs=[pl.BlockSpec(memory_space=pltpu.SMEM)] + [anywhere] * 6,
        out_specs=pl.BlockSpec(memory_space=pltpu.VMEM),
        scratch_shapes=[
            pltpu.VMEM((16, KROWS, ROWS), bf16),
            pltpu.VMEM((4, ROWS, QWIDTH), bf16),
            pltpu.VMEM((4, 16, 128), bf16),
            pltpu.VMEM((512, 512), bf16),
            pltpu.VMEM((512, 512), bf16),
            pltpu.VMEM((512, 2048), bf16),
            pltpu.VMEM((4, HEADS_DEV * ROWS, WIDTH), bf16),
            pltpu.VMEM((4, ROWS, 128), f32),
            pltpu.VMEM((4, HEADS_DEV, ROWS, 16 * ROWS), f32),
            pltpu.VMEM((4, HEADS_DEV, ROWS, 128), f32),
            pltpu.VMEM((R, 4, SUB, 512), bf16),
            pltpu.VMEM((R, 8, 128), f32),
            pltpu.VMEM((R, 3, SUB, 512), bf16),
            pltpu.VMEM((R, 3, 8, 128), f32),
            pltpu.VMEM((R, 4, SUB, 512), bf16),
            pltpu.VMEM((R, 2, SUB, 256), bf16),
            pltpu.VMEM((R, 2, SUB, 512), bf16),
            pltpu.VMEM((R, 2, SUB, 512), bf16),
            dma((6,)),
            dma((len(set(KEY_SEM.values())),)),
            dma((3, 2)),
            dma((3,)),
            dma((R,)),
            dma((R,)),
            dma((R, 3)),
            dma((7,)),
        ],
        compiler_params=pltpu.CompilerParams(
            collective_id=0, has_side_effects=True, vmem_limit_bytes=48 * 2**20
        ),
    )(*(
        pltpu.with_memory_space_constraint(a, pltpu.HBM)
        for a in (span_ids, query_nope, query_rope, cache.T, key_up, value_up, out_proj)
    ))


def solution(mesh):
    rows = ("outer", "inner")
    return jax.shard_map(
        shards,
        mesh=mesh,
        in_specs=(
            P(rows, "head"),
            P(rows, "head"),
            P(rows, None),
            P(rows),
            P(None, "head"),
            P(None, "head"),
            P("head", None),
        ),
        out_specs=P(rows, "head"),
        check_vma=False,
    )
```

```python
import jax
import jax.numpy as jnp
from jax import lax
from jax.experimental import pallas as pl
from jax.experimental.pallas import tpu as pltpu
from jax.sharding import PartitionSpec as P

LATENT = 512
ROPE = 64
NOPE = 128
SPAN = 64
HEADS_DEV = 4
ROWS = 128
WIDTH = LATENT + ROPE
QK = NOPE + ROPE
QWIDTH = HEADS_DEV * (NOPE + ROPE)
R = 4
SUB = ROWS // R
KROWS = WIDTH + 16
PIECES = ((0, 144), (144, 144), (288, 144), (432, 160))
SCALE = (NOPE + ROPE) ** -0.5 * 1.4426950408889634
LOG2E = 1.4426950408889634
LOWEST = -1e30
MESH = pl.DeviceIdType.MESH
NN = (((1,), (0,)), ((), ()))
f32 = jnp.float32
bf16 = jnp.bfloat16
BOTH = (4, 5, 6, 7, 12, 13, 14, 15)
KEY_SEM = {}
for _slot in range(1, 16):
    for _p in range(4):
        if _slot in BOTH and _p:
            KEY_SEM[_slot, _p] = KEY_SEM[_slot, 0]
        else:
            KEY_SEM[_slot, _p] = len(set(KEY_SEM.values()))
CHUNKS = ((0, 4, 8, 12), (1, 3, 5, 7), (2, 6, 9, 11), (10, 13, 14, 15))


def kernel(
    span_ref, qn_ref, qr_ref, k_ref, ku_ref, vu_ref, op_ref, out_ref,
    kbuf, qx, qpos, ku, vu, op, wk, kt, v_sc, qs, qc, s_sc, m_sc, pbuf, stat, rbuf, rstat,
    ybuf, y1, ysum, y2,
    load_sem, kr_sem, qr_sem, pr_sem, rr_sem, tr_sem, zr_sem, send_sem,
):
    h = lax.axis_index("head")
    o = lax.axis_index("outer")
    i = lax.axis_index("inner")
    zl, c = o // 2, o % 2
    y, x = i // 4, i % 4
    z = h * 2 + zl

    def at_z(zz):
        return (zz // 2, (zz % 2) * 2 + c, i)

    sib = (h, zl * 2 + 1 - c, i)
    yp = (h, o, ((y + 1) % 4) * 4 + x)
    ym = (h, o, ((y + 3) % 4) * 4 + x)
    zp = at_z((z + 1) % 8)
    zm = at_z((z + 7) % 8)
    xs = [None] + [(h, o, y * 4 + (x + d) % 4) for d in (1, 2, 3)]
    hp = ((h + 1) % 4, o, i)
    hm = ((h + 3) % 4, o, i)

    loads = [
        pltpu.make_async_copy(k_ref, kbuf.at[0, pl.ds(0, WIDTH)], load_sem.at[0]),
        pltpu.make_async_copy(qn_ref, qx.at[0, :, pl.ds(0, 512)], load_sem.at[1]),
        pltpu.make_async_copy(qr_ref, qx.at[0, :, pl.ds(512, 256)], load_sem.at[2]),
        pltpu.make_async_copy(ku_ref, ku, load_sem.at[3]),
        pltpu.make_async_copy(vu_ref, vu, load_sem.at[4]),
        pltpu.make_async_copy(op_ref, op, load_sem.at[5]),
    ]
    barrier = pltpu.get_barrier_semaphore()
    near = (sib, yp, ym, zp, zm, xs[1], xs[3])
    for partner in near:
        pl.semaphore_signal(barrier, inc=1, device_id=partner, device_id_type=MESH)
    for copy in loads:
        copy.start()
    first = span_ref[0].astype(f32)
    second = span_ref[1].astype(f32)
    lane = lax.broadcasted_iota(jnp.int32, (16, 128), 1)
    row = lax.broadcasted_iota(jnp.int32, (16, 128), 0)
    kbuf[0, WIDTH:KROWS, :] = jnp.where(lane < SPAN, first, second).astype(bf16)
    qpos[0] = jnp.where(row < 8, first, second).astype(bf16)
    loads[0].wait()
    pl.semaphore_wait(barrier, len(near))

    def send(src, dst, kind, r_sem, device):
        pltpu.make_async_remote_copy(
            src_ref=src, dst_ref=dst, send_sem=send_sem.at[kind], recv_sem=r_sem,
            device_id=device, device_id_type=MESH,
        ).start()

    def arrived(ref, sem):
        pltpu.make_async_copy(ref, ref, sem).wait()

    def piece(slot, p):
        begin, size = PIECES[p]
        return kbuf.at[slot, pl.ds(begin, size)]

    def send_k(slot, p, there, device):
        send(piece(slot, p), piece(there, p), 0, kr_sem.at[KEY_SEM[there, p]], device)

    def to_sib(slot):
        send(kbuf.at[slot], kbuf.at[slot + 4], 0, kr_sem.at[KEY_SEM[slot + 4, 0]], sib)

    def wait_k(slot, p=None):
        if p is None:
            arrived(kbuf.at[slot], kr_sem.at[KEY_SEM[slot, 0]])
        else:
            arrived(piece(slot, p), kr_sem.at[KEY_SEM[slot, p]])

    def qpart(slot, b):
        return qx.at[slot, pl.ds(b * SPAN, SPAN)]

    def send_q(slot, b, there, device):
        send(qpart(slot, b), qpart(there, b), 1, qr_sem.at[there - 1, b], device)

    def wait_q(slot, b):
        arrived(qpart(slot, b), qr_sem.at[slot - 1, b])

    def send_pos(slot, there, device):
        send(qpos.at[slot], qpos.at[there], 2, pr_sem.at[there - 1], device)

    def wait_pos(slot):
        arrived(qpos.at[slot], pr_sem.at[slot - 1])

    for p in (0, 1):
        send_k(0, p, 3, yp)
        send_k(0, p + 2, 1, ym)
        send_k(0, p, 8, zp)
        send_k(0, p + 2, 8, zm)
    to_sib(0)
    send_pos(0, 3, xs[1])
    send_pos(0, 1, xs[3])
    loads[1].wait()
    loads[2].wait()
    send_q(0, 0, 3, xs[1])
    send_q(0, 1, 1, xs[3])
    for p in (0, 1):
        send_k(0, p + 2, 3, yp)
        send_k(0, p, 1, ym)
    send_q(0, 1, 3, xs[1])
    send_q(0, 0, 1, xs[3])

    within = lax.rem(lax.broadcasted_iota(jnp.int32, (ROWS, 128), 0), SPAN).astype(f32)

    def build_q(d):
        for head in range(HEADS_DEV):
            mine = slice(d * ROWS, (d + 1) * ROWS)
            qs[head, mine, 0:NOPE] = qx[d, :, head * NOPE : (head + 1) * NOPE]
            begin = HEADS_DEV * NOPE + head * ROPE
            qs[head, mine, NOPE:QK] = qx[d, :, begin : begin + ROPE]
        spans = qpos[d].astype(f32)
        span = jnp.concatenate(
            [jnp.broadcast_to(spans[v : v + 1, :], (SPAN, 128)) for v in (0, 8)], axis=0
        )
        qc[d] = span * SPAN + within

    offset = lax.rem(lax.broadcasted_iota(jnp.int32, (1, 128), 1), SPAN).astype(f32)

    def lift(chunk):
        slots = CHUNKS[chunk]
        where = slice(chunk * 512, (chunk + 1) * 512)
        latents = jnp.concatenate([kbuf[s, 0:LATENT, :] for s in slots], axis=1)
        keys = lax.dot_general(wk[...], latents, NN, preferred_element_type=f32).astype(bf16)
        ropes = jnp.concatenate([kbuf[s, LATENT:WIDTH, :] for s in slots], axis=1)
        for head in range(HEADS_DEV):
            kt[head, 0:NOPE, where] = keys[head * NOPE : (head + 1) * NOPE]
            kt[head, NOPE:QK, where] = ropes
        v_sc[where, :] = lax.dot_general(
            latents, vu[...], (((0,), (0,)), ((), ())), preferred_element_type=f32
        ).astype(bf16)

    def masked(values, slot, rowpos):
        keypos = kbuf[slot, WIDTH:KROWS, :].astype(f32)[0:1, :] * SPAN + offset
        return jnp.where(keypos <= rowpos, values * SCALE, LOWEST)

    def scores(chunk, sources):
        for head in range(HEADS_DEV):
            queries = jnp.concatenate(
                [qs[head, d * ROWS : (d + 1) * ROWS, :] for d in sources], axis=0
            )
            values = lax.dot_general(
                queries, kt[head, :, chunk * 512 : (chunk + 1) * 512], NN,
                preferred_element_type=f32,
            )
            for n, d in enumerate(sources):
                rowpos = qc[d]
                peak = m_sc[d, head] if chunk else None
                for j, slot in enumerate(CHUNKS[chunk]):
                    part = values[n * ROWS : (n + 1) * ROWS, j * 128 : (j + 1) * 128]
                    part = masked(part, slot, rowpos)
                    begin = chunk * 512 + j * 128
                    s_sc[d, head, :, begin : begin + 128] = part
                    peak = part if peak is None else jnp.maximum(peak, part)
                m_sc[d, head] = peak

    build_q(0)
    loads[3].wait()
    wk[...] = jnp.transpose(ku[...])
    for p in (0, 1):
        wait_k(3, p)
        send_k(3, p, 2, yp)
        send_k(3, p, 11, zp)
        wait_k(1, p + 2)
        send_k(1, p + 2, 2, ym)
        send_k(1, p + 2, 9, zm)
    wait_q(3, 0)
    send_q(3, 0, 2, xs[1])
    wait_q(1, 1)
    send_q(1, 1, 2, xs[3])
    wait_pos(3)
    send_pos(3, 2, xs[1])
    wait_pos(1)
    for p in range(4):
        wait_k(8, p)
    to_sib(8)
    for p in (0, 1):
        wait_k(3, p + 2)
        send_k(3, p + 2, 11, zm)
        wait_k(1, p)
        send_k(1, p, 9, zp)
    to_sib(3)
    to_sib(1)
    loads[4].wait()
    wait_k(4)
    wait_k(12)
    lift(0)
    for p in (0, 1):
        wait_k(2, p)
        send_k(2, p, 10, zp)
        wait_k(2, p + 2)
        send_k(2, p + 2, 10, zm)
    to_sib(2)
    scores(0, (0,))
    wait_q(3, 1)
    build_q(3)
    wait_q(1, 0)
    build_q(1)
    scores(0, (3, 1))
    wait_k(5)
    wait_k(7)
    lift(1)
    scores(1, (0, 3, 1))
    for slot in (11, 9):
        for p in range(4):
            wait_k(slot, p)
        to_sib(slot)
    for b in (0, 1):
        wait_q(2, b)
    wait_pos(2)
    build_q(2)
    scores(0, (2,))
    for p in range(4):
        wait_k(10, p)
    to_sib(10)
    scores(1, (2,))
    wait_k(6)
    lift(2)
    scores(2, (0, 1, 2, 3))
    wait_k(13)
    wait_k(15)
    wait_k(14)
    lift(3)

    def weigh(r):
        rows = slice(r * SUB, (r + 1) * SUB)
        heads = range(HEADS_DEV)
        rowpos = qc[:, rows, :].reshape(4 * SUB, 128)
        scored, tops = [], []
        for head in heads:
            queries = jnp.concatenate(
                [qs[head, d * ROWS + r * SUB : d * ROWS + (r + 1) * SUB, :] for d in range(4)],
                axis=0,
            )
            scored.append(
                lax.dot_general(queries, kt[head, :, 1536:2048], NN, preferred_element_type=f32)
            )
        for head in heads:
            peak = m_sc[:, head, rows, :].reshape(4 * SUB, 128)
            for j, slot in enumerate(CHUNKS[3]):
                part = masked(scored[head][:, j * 128 : (j + 1) * 128], slot, rowpos)
                s_sc[:, head, rows, 1536 + j * 128 : 1664 + j * 128] = part.reshape(4, SUB, 128)
                peak = jnp.maximum(peak, part)
            tops.append(jnp.max(peak, axis=1, keepdims=True))
        totals, accs = [], []
        for head in heads:
            wide = jnp.broadcast_to(tops[head], (4 * SUB, 128))
            total = None
            parts = []
            for n in range(16):
                value = s_sc[:, head, rows, n * 128 : (n + 1) * 128].reshape(4 * SUB, 128)
                w = jnp.exp2(value - wide)
                total = w if total is None else total + w
                parts.append(w.astype(bf16))
            totals.append(total)
            accs.append(lax.dot_general(
                jnp.concatenate(parts, axis=1), v_sc[:, head * 128 : (head + 1) * 128], NN,
                preferred_element_type=f32,
            ))
        denoms = [jnp.sum(total, axis=1, keepdims=True) for total in totals]
        logs = [top + jnp.log(denom) * LOG2E for top, denom in zip(tops, denoms)]
        outs = [(acc * (1.0 / denom)).astype(bf16) for acc, denom in zip(accs, denoms)]
        for head in range(HEADS_DEV):
            for d in range(4):
                pbuf[r, d, :, head * 128 : (head + 1) * 128] = outs[head][d * SUB : (d + 1) * SUB]
            flat = jnp.transpose(jnp.broadcast_to(logs[head], (128, 128)))
            stat[r, head : head + 1, :] = flat[0:1, :]
        for d in (2, 1, 3):
            send(pbuf.at[r, d], rbuf.at[r, d - 1], 3, rr_sem.at[r], xs[d])
            send(stat.at[r], rstat.at[r, d - 1], 4, tr_sem.at[r], xs[d])

    def merge(r):
        arrived(rstat.at[r], tr_sem.at[r])
        arrived(rbuf.at[r], rr_sem.at[r])
        tiles = [stat[r]] + [rstat[r, d] for d in range(3)]
        columns = [
            jnp.transpose(tile)[d * SUB : (d + 1) * SUB, :] for d, tile in enumerate(tiles)
        ]
        heads = []
        for head in range(HEADS_DEV):
            logs = [col[:, head : head + 1] for col in columns]
            top = jnp.maximum(jnp.maximum(logs[0], logs[1]), jnp.maximum(logs[2], logs[3]))
            scale = [jnp.exp2(v - top) for v in logs]
            total = scale[0] + scale[1] + scale[2] + scale[3]
            where = slice(head * 128, (head + 1) * 128)
            acc = pbuf[r, 0, :, where].astype(f32) * scale[0]
            for d in range(3):
                acc = acc + rbuf[r, d, :, where].astype(f32) * scale[d + 1]
            heads.append((acc / total).astype(bf16))
        head_out = jnp.concatenate(heads, axis=1)
        for d in (2, 1, 3, 0):
            begin = pl.multiple_of(((h + d) % 4) * 512, 512)
            ybuf[r, d] = lax.dot_general(
                head_out, op[:, pl.ds(begin, 512)], NN, preferred_element_type=f32
            ).astype(bf16)
            if d == 2:
                send(
                    ybuf.at[r, 2, :, pl.ds(0, 256)], y1.at[r, 0], 5, zr_sem.at[r, 0], hp,
                )
                send(
                    ybuf.at[r, 2, :, pl.ds(256, 256)], y1.at[r, 1], 5, zr_sem.at[r, 1], hm,
                )

    def pass_on(r):
        arrived(y1.at[r, 0], zr_sem.at[r, 0])
        left = ybuf[r, 1, :, 0:256].astype(f32) + y1[r, 0].astype(f32)
        ysum[r, 0, :, 0:256] = left.astype(bf16)
        ysum[r, 0, :, 256:512] = ybuf[r, 1, :, 256:512]
        send(ysum.at[r, 0], y2.at[r, 0], 6, zr_sem.at[r, 2], hp)
        arrived(y1.at[r, 1], zr_sem.at[r, 1])
        right = ybuf[r, 3, :, 256:512].astype(f32) + y1[r, 1].astype(f32)
        ysum[r, 1, :, 256:512] = right.astype(bf16)
        ysum[r, 1, :, 0:256] = ybuf[r, 3, :, 0:256]
        send(ysum.at[r, 1], y2.at[r, 1], 6, zr_sem.at[r, 2], hm)

    def finish(r):
        arrived(y2.at[r], zr_sem.at[r, 2])
        total = ybuf[r, 0].astype(f32) + y2[r, 0].astype(f32) + y2[r, 1].astype(f32)
        out_ref[r * SUB : (r + 1) * SUB, :] = total.astype(bf16)

    for r in range(R):
        weigh(r)
    loads[5].wait()
    for r in range(R):
        merge(r)
    for r in range(R):
        pass_on(r)
    for r in range(R):
        finish(r)
    for kind, ref in enumerate((
        kbuf.at[pl.ds(0, 15)], qx.at[pl.ds(0, 3)], qpos.at[pl.ds(0, 3)], rbuf, rstat, y1, y2,
    )):
        arrived(ref, send_sem.at[kind])


def shards(query_nope, query_rope, cache, span_ids, key_up, value_up, out_proj):
    anywhere = pl.BlockSpec(memory_space=pl.ANY)
    dma = pltpu.SemaphoreType.DMA
    return pl.pallas_call(
        kernel,
        name="attend",
        out_shape=jax.ShapeDtypeStruct((ROWS, 512), bf16),
        in_specs=[pl.BlockSpec(memory_space=pltpu.SMEM)] + [anywhere] * 6,
        out_specs=pl.BlockSpec(memory_space=pltpu.VMEM),
        scratch_shapes=[
            pltpu.VMEM((16, KROWS, ROWS), bf16),
            pltpu.VMEM((4, ROWS, QWIDTH), bf16),
            pltpu.VMEM((4, 16, 128), bf16),
            pltpu.VMEM((512, 512), bf16),
            pltpu.VMEM((512, 512), bf16),
            pltpu.VMEM((512, 2048), bf16),
            pltpu.VMEM((512, LATENT), bf16),
            pltpu.VMEM((HEADS_DEV, QK, 16 * ROWS), bf16),
            pltpu.VMEM((16 * ROWS, 512), bf16),
            pltpu.VMEM((HEADS_DEV, 4 * ROWS, QK), bf16),
            pltpu.VMEM((4, ROWS, 128), f32),
            pltpu.VMEM((4, HEADS_DEV, ROWS, 16 * ROWS), f32),
            pltpu.VMEM((4, HEADS_DEV, ROWS, 128), f32),
            pltpu.VMEM((R, 4, SUB, 512), bf16),
            pltpu.VMEM((R, 8, 128), f32),
            pltpu.VMEM((R, 3, SUB, 512), bf16),
            pltpu.VMEM((R, 3, 8, 128), f32),
            pltpu.VMEM((R, 4, SUB, 512), bf16),
            pltpu.VMEM((R, 2, SUB, 256), bf16),
            pltpu.VMEM((R, 2, SUB, 512), bf16),
            pltpu.VMEM((R, 2, SUB, 512), bf16),
            dma((6,)),
            dma((len(set(KEY_SEM.values())),)),
            dma((3, 2)),
            dma((3,)),
            dma((R,)),
            dma((R,)),
            dma((R, 3)),
            dma((7,)),
        ],
        compiler_params=pltpu.CompilerParams(
            collective_id=0, has_side_effects=True, vmem_limit_bytes=48 * 2**20
        ),
    )(*(
        pltpu.with_memory_space_constraint(a, pltpu.HBM)
        for a in (span_ids, query_nope, query_rope, cache.T, key_up, value_up, out_proj)
    ))


def solution(mesh):
    rows = ("outer", "inner")
    return jax.shard_map(
        shards,
        mesh=mesh,
        in_specs=(
            P(rows, "head"),
            P(rows, "head"),
            P(rows, None),
            P(rows),
            P(None, "head"),
            P(None, "head"),
            P("head", None),
        ),
        out_specs=P(rows, "head"),
        check_vma=False,
    )
```

```python
import jax
import jax.numpy as jnp
from jax import lax
from jax.experimental import pallas as pl
from jax.experimental.pallas import tpu as pltpu
from jax.sharding import PartitionSpec as P

LATENT = 512
ROPE = 64
NOPE = 128
SPAN = 64
HEADS_DEV = 4
ROWS = 128
WIDTH = LATENT + ROPE
QK = NOPE + ROPE
QWIDTH = HEADS_DEV * (NOPE + ROPE)
PARTS = ((0, 16), (16, 32), (48, 32), (80, 32), (112, 16))
R = len(PARTS)
DEEP = 256
KROWS = WIDTH + 16
PIECES = ((0, 144), (144, 144), (288, 144), (432, 160))
SCALE = (NOPE + ROPE) ** -0.5 * 1.4426950408889634
LOG2E = 1.4426950408889634
LOWEST = -1e30
ARRIVAL = (0, 3, 1, 2)
MESH = pl.DeviceIdType.MESH
NN = (((1,), (0,)), ((), ()))
f32 = jnp.float32
bf16 = jnp.bfloat16
BOTH = (4, 5, 6, 7, 12, 13, 14, 15)
KEY_SEM = {}
for _slot in range(1, 16):
    for _p in range(4):
        if _slot in BOTH and _p:
            KEY_SEM[_slot, _p] = KEY_SEM[_slot, 0]
        else:
            KEY_SEM[_slot, _p] = len(set(KEY_SEM.values()))
CHUNKS = ((0, 4), (8, 12), (1, 5, 3, 7), (2, 6, 9, 11), (13, 15, 10, 14))
STARTS = (0, 256, 512, 1024, 1536)
LAST = len(CHUNKS) - 1


def kernel(
    span_ref, qn_ref, qr_ref, k_ref, ku_ref, vu_ref, op_ref, out_ref,
    kbuf, qx, qpos, ku, vu, op, wk, kt, v_sc, qs, qspan, s_sc, m_sc, pbuf, stat, rbuf, rstat,
    ybuf, y1, ysum, y2, y3,
    load_sem, kr_sem, qr_sem, pr_sem, rr_sem, tr_sem, zr_sem, send_sem,
):
    h = lax.axis_index("head")
    o = lax.axis_index("outer")
    i = lax.axis_index("inner")
    zl, c = o // 2, o % 2
    y, x = i // 4, i % 4
    z = h * 2 + zl

    def at_z(zz):
        return (zz // 2, (zz % 2) * 2 + c, i)

    sib = (h, zl * 2 + 1 - c, i)
    yp = (h, o, ((y + 1) % 4) * 4 + x)
    ym = (h, o, ((y + 3) % 4) * 4 + x)
    zp = at_z((z + 1) % 8)
    zm = at_z((z + 7) % 8)
    xs = [None] + [(h, o, y * 4 + (x + d) % 4) for d in (1, 2, 3)]
    hp = ((h + 1) % 4, o, i)
    hm = ((h + 3) % 4, o, i)
    far = ((h + 2) % 4, o, i)

    loads = [
        pltpu.make_async_copy(k_ref, kbuf.at[0, pl.ds(0, WIDTH)], load_sem.at[0]),
        pltpu.make_async_copy(qn_ref, qx.at[0, :, pl.ds(0, 512)], load_sem.at[1]),
        pltpu.make_async_copy(qr_ref, qx.at[0, :, pl.ds(512, 256)], load_sem.at[2]),
        pltpu.make_async_copy(ku_ref, ku, load_sem.at[3]),
        pltpu.make_async_copy(vu_ref, vu, load_sem.at[4]),
        pltpu.make_async_copy(op_ref, op, load_sem.at[5]),
    ]
    barrier = pltpu.get_barrier_semaphore()
    near = (sib, yp, ym, zp, zm, xs[1], xs[3])
    for partner in near:
        pl.semaphore_signal(barrier, inc=1, device_id=partner, device_id_type=MESH)
    for copy in loads:
        copy.start()
    first = span_ref[0].astype(f32)
    second = span_ref[1].astype(f32)
    lane = lax.broadcasted_iota(jnp.int32, (16, 128), 1)
    row = lax.broadcasted_iota(jnp.int32, (16, 128), 0)
    kbuf[0, WIDTH:KROWS, :] = jnp.where(lane < SPAN, first, second).astype(bf16)
    qpos[0] = jnp.where(row < 8, first, second).astype(bf16)
    kt[:, QK:DEEP, :] = jnp.zeros((HEADS_DEV, DEEP - QK, 16 * ROWS), bf16)
    loads[0].wait()
    pl.semaphore_wait(barrier, len(near))

    def send(src, dst, kind, r_sem, device):
        pltpu.make_async_remote_copy(
            src_ref=src, dst_ref=dst, send_sem=send_sem.at[kind], recv_sem=r_sem,
            device_id=device, device_id_type=MESH,
        ).start()

    def arrived(ref, sem):
        pltpu.make_async_copy(ref, ref, sem).wait()

    def piece(slot, p):
        begin, size = PIECES[p]
        return kbuf.at[slot, pl.ds(begin, size)]

    def send_k(slot, p, there, device):
        send(piece(slot, p), piece(there, p), 0, kr_sem.at[KEY_SEM[there, p]], device)

    def to_sib(slot):
        send(kbuf.at[slot], kbuf.at[slot + 4], 0, kr_sem.at[KEY_SEM[slot + 4, 0]], sib)

    def wait_k(slot, p=None):
        if p is None:
            arrived(kbuf.at[slot], kr_sem.at[KEY_SEM[slot, 0]])
        else:
            arrived(piece(slot, p), kr_sem.at[KEY_SEM[slot, p]])

    def qpart(slot, b):
        return qx.at[slot, pl.ds(b * SPAN, SPAN)]

    def send_q(slot, b, there, device):
        send(qpart(slot, b), qpart(there, b), 1, qr_sem.at[there - 1, b], device)

    def wait_q(slot, b):
        arrived(qpart(slot, b), qr_sem.at[slot - 1, b])

    def send_pos(slot, there, device):
        send(qpos.at[slot], qpos.at[there], 2, pr_sem.at[there - 1], device)

    def wait_pos(slot):
        arrived(qpos.at[slot], pr_sem.at[slot - 1])

    for p in (0, 1):
        send_k(0, p, 3, yp)
        send_k(0, p + 2, 1, ym)
        send_k(0, p, 8, zp)
        send_k(0, p + 2, 8, zm)
    to_sib(0)
    send_pos(0, 3, xs[1])
    send_pos(0, 1, xs[3])
    loads[1].wait()
    loads[2].wait()
    send_q(0, 0, 3, xs[1])
    send_q(0, 1, 1, xs[3])
    for p in (0, 1):
        send_k(0, p + 2, 3, yp)
        send_k(0, p, 1, ym)
    send_q(0, 1, 3, xs[1])
    send_q(0, 0, 1, xs[3])

    column = lax.broadcasted_iota(jnp.int32, (ROWS, ROPE), 1)
    late = lax.broadcasted_iota(jnp.int32, (ROWS, ROPE), 0) // SPAN

    def build_q(k):
        d = ARRIVAL[k]
        for head in range(HEADS_DEV):
            qs[head, k, :, 0:NOPE] = qx[d, :, head * NOPE : (head + 1) * NOPE]
            begin = HEADS_DEV * NOPE + head * ROPE
            qs[head, k, :, NOPE:QK] = qx[d, :, begin : begin + ROPE]
            qs[head, k, :, QK:DEEP] = jnp.where(column == 2 * k + late, 1.0, 0.0).astype(bf16)
        spans = qpos[d].astype(f32)
        qspan[2 * k : 2 * k + 1, :] = spans[0:1, :]
        qspan[2 * k + 1 : 2 * k + 2, :] = spans[8:9, :]

    def columns(chunk):
        return slice(STARTS[chunk], STARTS[chunk] + ROWS * len(CHUNKS[chunk]))

    def later(chunk, first=0, count=4):
        for j, slot in enumerate(CHUNKS[chunk]):
            if not first <= j < first + count:
                continue
            begin = STARTS[chunk] + j * ROWS
            span = kbuf[slot, WIDTH:KROWS, :].astype(f32)[0:8, :]
            bias = jnp.where(span > qspan[...], LOWEST, 0.0)
            bias = jnp.concatenate([bias, jnp.zeros((8, 128), f32)], axis=0).astype(bf16)
            for head in range(HEADS_DEV):
                kt[head, QK : QK + 16, begin : begin + ROWS] = bias

    def lift(chunk, first=0, count=4):
        slots = CHUNKS[chunk][first : first + count]
        begin = STARTS[chunk] + first * ROWS
        where = slice(begin, begin + len(slots) * ROWS)
        latents = jnp.concatenate([kbuf[s, 0:LATENT, :] for s in slots], axis=1)
        keys = lax.dot_general(wk[...], latents, NN, preferred_element_type=f32).astype(bf16)
        ropes = jnp.concatenate([kbuf[s, LATENT:WIDTH, :] for s in slots], axis=1)
        for head in range(HEADS_DEV):
            kt[head, 0:NOPE, where] = keys[head * NOPE : (head + 1) * NOPE]
            kt[head, NOPE:QK, where] = ropes
        v_sc[where, :] = lax.dot_general(
            latents, vu[...], (((0,), (0,)), ((), ())), preferred_element_type=f32
        ).astype(bf16)
        later(chunk, first, count)

    rowid = lax.broadcasted_iota(jnp.int32, (ROWS, ROWS), 0)
    keyid = lax.broadcasted_iota(jnp.int32, (ROWS, ROWS), 1)
    ahead = (keyid > rowid) & (keyid // SPAN == rowid // SPAN)

    def scores(chunk, low, high):
        count = (high - low) * ROWS
        size = len(CHUNKS[chunk])
        for head in range(HEADS_DEV):
            values = lax.dot_general(
                qs[head, low:high].reshape(count, DEEP), kt[head, :, columns(chunk)], NN,
                preferred_element_type=f32,
            )
            peak = m_sc[head, low:high].reshape(count, 128) if chunk else None
            for j in range(size):
                part = values[:, j * 128 : (j + 1) * 128] * SCALE
                if chunk == 0 and low == 0 and j == 0:
                    part = jnp.where(ahead, LOWEST, part)
                begin = STARTS[chunk] + j * 128
                s_sc[head, low:high, :, begin : begin + 128] = part.reshape(high - low, ROWS, 128)
                peak = part if peak is None else jnp.maximum(peak, part)
            m_sc[head, low:high] = peak.reshape(high - low, ROWS, 128)

    build_q(0)
    loads[3].wait()
    wk[...] = jnp.transpose(ku[...])
    loads[4].wait()
    wait_k(4)
    lift(0)
    scores(0, 0, 1)
    for p in (0, 1):
        wait_k(3, p)
        send_k(3, p, 2, yp)
        send_k(3, p, 11, zp)
        wait_k(1, p + 2)
        send_k(1, p + 2, 2, ym)
        send_k(1, p + 2, 9, zm)
    for p in (0, 1):
        wait_k(8, p)
        send_k(8, p, 9, ym)
        wait_k(8, p + 2)
        send_k(8, p + 2, 11, yp)
    to_sib(8)
    wait_q(3, 0)
    send_q(3, 0, 2, xs[1])
    wait_q(1, 1)
    send_q(1, 1, 2, xs[3])
    wait_pos(3)
    send_pos(3, 2, xs[1])
    wait_pos(1)
    for p in (0, 1):
        wait_k(3, p + 2)
        wait_k(1, p)
    to_sib(3)
    to_sib(1)
    wait_k(12)
    lift(1)
    scores(1, 0, 1)
    for p in (0, 1):
        wait_k(2, p)
        send_k(2, p, 10, zp)
        wait_k(2, p + 2)
        send_k(2, p + 2, 10, zm)
    to_sib(2)
    wait_q(3, 1)
    build_q(1)
    wait_q(1, 0)
    build_q(2)
    later(0)
    later(1)
    scores(0, 1, 3)
    scores(1, 1, 3)
    wait_k(5)
    wait_k(7)
    lift(2)
    scores(2, 0, 3)
    for slot in (11, 9):
        for p in range(4):
            wait_k(slot, p)
        to_sib(slot)
    for b in (0, 1):
        wait_q(2, b)
    wait_pos(2)
    build_q(3)
    for chunk in range(3):
        later(chunk)
    scores(0, 3, 4)
    scores(1, 3, 4)
    scores(2, 3, 4)
    wait_k(6)
    lift(3)
    for p in range(4):
        wait_k(10, p)
    to_sib(10)
    scores(3, 0, 4)
    wait_k(13)
    wait_k(15)
    lift(LAST, 0, 2)
    wait_k(14)
    lift(LAST, 2, 2)

    def weigh(r):
        begin, size = PARTS[r]
        rows = slice(begin, begin + size)
        count = 4 * size
        heads = range(HEADS_DEV)
        scored = [
            lax.dot_general(
                qs[head, :, rows, :].reshape(count, DEEP), kt[head, :, columns(LAST)], NN,
                preferred_element_type=f32,
            )
            for head in heads
        ]
        kept = STARTS[LAST] // 128
        fresh, peaks = [], []
        for head in heads:
            peak = m_sc[head, :, rows, :].reshape(count, 128)
            parts = []
            for j in range(len(CHUNKS[LAST])):
                parts.append(scored[head][:, j * 128 : (j + 1) * 128] * SCALE)
                peak = jnp.maximum(peak, parts[-1])
            fresh.append(parts)
            peaks.append(jnp.broadcast_to(jnp.max(peak, axis=1, keepdims=True), (count, 128)))
        results = []
        for head in heads:
            total = None
            ws = []
            for n in range(16):
                if n < kept:
                    part = s_sc[head, :, rows, n * 128 : (n + 1) * 128].reshape(count, 128)
                else:
                    part = fresh[head][n - kept]
                w = jnp.exp2(part - peaks[head])
                total = w if total is None else total + w
                ws.append(w.astype(bf16))
            out = lax.dot_general(
                jnp.concatenate(ws, axis=1), v_sc[:, head * 128 : (head + 1) * 128], NN,
                preferred_element_type=f32,
            )
            results.append((peaks[head], total, out))
        denoms = [jnp.sum(total, axis=1, keepdims=True) for _, total, _ in results]
        for head, (peak, _, out) in enumerate(results):
            part = (out * (1.0 / denoms[head])).astype(bf16)
            for k, d in enumerate(ARRIVAL):
                pbuf[d, rows, head * 128 : (head + 1) * 128] = part[k * size : (k + 1) * size]
            log = peak + jnp.broadcast_to(jnp.log(denoms[head]) * LOG2E, (4 * size, 128))
            log = jnp.concatenate([log] * (32 // size), axis=0)
            stat[r, head : head + 1, :] = jnp.transpose(log)[0:1, :]
        here = pl.ds(begin, size)
        for d in (2, 1, 3):
            send(pbuf.at[d, here], rbuf.at[d - 1, here], 3, rr_sem.at[r], xs[d])
            send(stat.at[r], rstat.at[r, d - 1], 4, tr_sem.at[r], xs[d])

    def merge(r):
        begin, size = PARTS[r]
        rows, here = slice(begin, begin + size), pl.ds(begin, size)
        arrived(rstat.at[r], tr_sem.at[r])
        arrived(rbuf.at[:, here], rr_sem.at[r])
        tiles = [stat[r]] + [rstat[r, d] for d in range(3)]
        tops = []
        for d, tile in enumerate(tiles):
            k = ARRIVAL.index(d)
            tops.append(jnp.transpose(jnp.concatenate([tile, tile], axis=0))[k * size : (k + 1) * size, :])
        heads = []
        for head in range(HEADS_DEV):
            logs = [col[:, head : head + 1] for col in tops]
            top = jnp.maximum(jnp.maximum(logs[0], logs[1]), jnp.maximum(logs[2], logs[3]))
            scale = [jnp.exp2(v - top) for v in logs]
            total = scale[0] + scale[1] + scale[2] + scale[3]
            where = slice(head * 128, (head + 1) * 128)
            acc = pbuf[0, rows, where].astype(f32) * scale[0]
            for d in range(3):
                acc = acc + rbuf[d, rows, where].astype(f32) * scale[d + 1]
            heads.append((acc * (1.0 / total)).astype(bf16))
        head_out = jnp.concatenate(heads, axis=1)
        low, high = pl.ds(0, 256), pl.ds(256, 256)
        mixed = []
        for d in (2, 1, 3, 0):
            start = pl.multiple_of(((h + d) % 4) * 512, 512)
            mixed.append(lax.dot_general(
                head_out, op[:, pl.ds(start, 512)], NN, preferred_element_type=f32
            ).astype(bf16))
        for d, y in zip((2, 1, 3, 0), mixed):
            ybuf[d, rows] = y
        if r == R - 1:
            send(ybuf.at[2, here], y3, 7, zr_sem.at[r, 0], far)
            send(ybuf.at[1, here], y2.at[0, here], 6, zr_sem.at[r, 2], hp)
            send(ybuf.at[3, here], y2.at[1, here], 6, zr_sem.at[r, 2], hm)
            return
        send(ybuf.at[2, here, low], y1.at[0, here], 5, zr_sem.at[r, 0], hp)
        send(ybuf.at[2, here, high], y1.at[1, here], 5, zr_sem.at[r, 1], hm)
        send(ybuf.at[1, here, high], y2.at[0, here, high], 6, zr_sem.at[r, 2], hp)
        send(ybuf.at[3, here, low], y2.at[1, here, low], 6, zr_sem.at[r, 2], hm)

    def pass_on(r):
        begin, size = PARTS[r]
        rows, here = slice(begin, begin + size), pl.ds(begin, size)
        low, high = pl.ds(0, 256), pl.ds(256, 256)
        arrived(y1.at[0, here], zr_sem.at[r, 0])
        left = ybuf[1, rows, 0:256].astype(f32) + y1[0, rows].astype(f32)
        ysum[0, rows] = left.astype(bf16)
        send(ysum.at[0, here], y2.at[0, here, low], 6, zr_sem.at[r, 2], hp)
        arrived(y1.at[1, here], zr_sem.at[r, 1])
        right = ybuf[3, rows, 256:512].astype(f32) + y1[1, rows].astype(f32)
        ysum[1, rows] = right.astype(bf16)
        send(ysum.at[1, here], y2.at[1, here, high], 6, zr_sem.at[r, 2], hm)

    def finish(r):
        begin, size = PARTS[r]
        rows, here = slice(begin, begin + size), pl.ds(begin, size)
        arrived(y2.at[:, here], zr_sem.at[r, 2])
        total = ybuf[0, rows].astype(f32) + y2[0, rows].astype(f32) + y2[1, rows].astype(f32)
        if r == R - 1:
            arrived(y3, zr_sem.at[r, 0])
            total = total + y3[...].astype(f32)
        out_ref[rows, :] = total.astype(bf16)

    weigh(0)
    weigh(1)
    weigh(2)
    weigh(3)
    loads[5].wait()
    merge(0)
    weigh(4)
    merge(1)
    merge(2)
    pass_on(0)
    merge(3)
    pass_on(1)
    merge(4)
    pass_on(2)
    pass_on(3)
    for r in range(R):
        finish(r)
    for kind, ref in enumerate((
        kbuf.at[pl.ds(0, 15)], qx.at[pl.ds(0, 3)], qpos.at[pl.ds(0, 3)], rbuf, rstat,
        y1.at[:, pl.ds(0, PARTS[-1][0])], y2, y3,
    )):
        arrived(ref, send_sem.at[kind])


def shards(query_nope, query_rope, cache, span_ids, key_up, value_up, out_proj):
    anywhere = pl.BlockSpec(memory_space=pl.ANY)
    dma = pltpu.SemaphoreType.DMA
    return pl.pallas_call(
        kernel,
        name="attend",
        out_shape=jax.ShapeDtypeStruct((ROWS, 512), bf16),
        in_specs=[pl.BlockSpec(memory_space=pltpu.SMEM)] + [anywhere] * 6,
        out_specs=pl.BlockSpec(memory_space=pltpu.VMEM),
        scratch_shapes=[
            pltpu.VMEM((16, KROWS, ROWS), bf16),
            pltpu.VMEM((4, ROWS, QWIDTH), bf16),
            pltpu.VMEM((4, 16, 128), bf16),
            pltpu.VMEM((512, 512), bf16),
            pltpu.VMEM((512, 512), bf16),
            pltpu.VMEM((512, 2048), bf16),
            pltpu.VMEM((512, LATENT), bf16),
            pltpu.VMEM((HEADS_DEV, DEEP, 16 * ROWS), bf16),
            pltpu.VMEM((16 * ROWS, 512), bf16),
            pltpu.VMEM((HEADS_DEV, 4, ROWS, DEEP), bf16),
            pltpu.VMEM((8, 128), f32),
            pltpu.VMEM((HEADS_DEV, 4, ROWS, 16 * ROWS), f32),
            pltpu.VMEM((HEADS_DEV, 4, ROWS, 128), f32),
            pltpu.VMEM((4, ROWS, 512), bf16),
            pltpu.VMEM((R, 4, 128), f32),
            pltpu.VMEM((3, ROWS, 512), bf16),
            pltpu.VMEM((R, 3, 4, 128), f32),
            pltpu.VMEM((4, ROWS, 512), bf16),
            pltpu.VMEM((2, ROWS, 256), bf16),
            pltpu.VMEM((2, ROWS, 256), bf16),
            pltpu.VMEM((2, ROWS, 512), bf16),
            pltpu.VMEM((PARTS[-1][1], 512), bf16),
            dma((6,)),
            dma((len(set(KEY_SEM.values())),)),
            dma((3, 2)),
            dma((3,)),
            dma((R,)),
            dma((R,)),
            dma((R, 3)),
            dma((8,)),
        ],
        compiler_params=pltpu.CompilerParams(
            collective_id=0, has_side_effects=True, vmem_limit_bytes=48 * 2**20
        ),
    )(*(
        pltpu.with_memory_space_constraint(a, pltpu.HBM)
        for a in (span_ids, query_nope, query_rope, cache.T, key_up, value_up, out_proj)
    ))


def solution(mesh):
    rows = ("outer", "inner")
    return jax.shard_map(
        shards,
        mesh=mesh,
        in_specs=(
            P(rows, "head"),
            P(rows, "head"),
            P(rows, None),
            P(rows),
            P(None, "head"),
            P(None, "head"),
            P("head", None),
        ),
        out_specs=P(rows, "head"),
        check_vma=False,
    )
```

```python
import jax
import jax.numpy as jnp
from jax import lax
from jax.experimental import pallas as pl
from jax.experimental.pallas import tpu as pltpu
from jax.sharding import PartitionSpec as P

LATENT = 512
ROPE = 64
NOPE = 128
SPAN = 64
HEADS_DEV = 4
ROWS = 128
WIDTH = LATENT + ROPE
QK = NOPE + ROPE
QWIDTH = HEADS_DEV * (NOPE + ROPE)
PARTS = ((0, 16), (16, 32), (48, 32), (80, 32), (112, 16))
R = len(PARTS)
DEEP = 256
KROWS = WIDTH + 16
PIECES = ((0, 96), (96, 96), (192, 96), (288, 96), (384, 96), (480, 112))
HALF = 3
SCALE = (NOPE + ROPE) ** -0.5 * 1.4426950408889634
LOG2E = 1.4426950408889634
LOWEST = -1e30
ARRIVAL = (0, 3, 1, 2)
MESH = pl.DeviceIdType.MESH
NN = (((1,), (0,)), ((), ()))
f32 = jnp.float32
bf16 = jnp.bfloat16
BOTH = (4, 5, 6, 7, 12, 13, 14, 15)
KEY_SEM = {}
for _slot in range(1, 16):
    for _p in range(2 * HALF):
        if _slot in BOTH and _p:
            KEY_SEM[_slot, _p] = KEY_SEM[_slot, 0]
        else:
            KEY_SEM[_slot, _p] = len(set(KEY_SEM.values()))
CHUNKS = ((0, 4), (8, 12), (1, 5, 3, 7), (2, 6, 9, 11), (13, 15, 10, 14))
STARTS = (0, 256, 512, 1024, 1536)
LAST = len(CHUNKS) - 1


def kernel(
    span_ref, qn_ref, qr_ref, k_ref, ku_ref, vu_ref, op_ref, out_ref,
    kbuf, qx, qpos, ku, vu, op, wk, kt, v_sc, qs, qspan, s_sc, m_sc, pbuf, stat, rbuf, rstat,
    ybuf, y1, ysum, y2, y3,
    load_sem, kr_sem, qr_sem, pr_sem, rr_sem, tr_sem, zr_sem, send_sem,
):
    h = lax.axis_index("head")
    o = lax.axis_index("outer")
    i = lax.axis_index("inner")
    zl, c = o // 2, o % 2
    y, x = i // 4, i % 4
    z = h * 2 + zl

    def at_z(zz):
        return (zz // 2, (zz % 2) * 2 + c, i)

    sib = (h, zl * 2 + 1 - c, i)
    yp = (h, o, ((y + 1) % 4) * 4 + x)
    ym = (h, o, ((y + 3) % 4) * 4 + x)
    zp = at_z((z + 1) % 8)
    zm = at_z((z + 7) % 8)
    xs = [None] + [(h, o, y * 4 + (x + d) % 4) for d in (1, 2, 3)]
    hp = ((h + 1) % 4, o, i)
    hm = ((h + 3) % 4, o, i)
    far = ((h + 2) % 4, o, i)

    loads = [
        pltpu.make_async_copy(k_ref, kbuf.at[0, pl.ds(0, WIDTH)], load_sem.at[0]),
        pltpu.make_async_copy(qn_ref, qx.at[0, :, pl.ds(0, 512)], load_sem.at[1]),
        pltpu.make_async_copy(qr_ref, qx.at[0, :, pl.ds(512, 256)], load_sem.at[2]),
        pltpu.make_async_copy(ku_ref, ku, load_sem.at[3]),
        pltpu.make_async_copy(vu_ref, vu, load_sem.at[4]),
        pltpu.make_async_copy(op_ref, op, load_sem.at[5]),
    ]
    barrier = pltpu.get_barrier_semaphore()
    near = (sib, yp, ym, zp, zm, xs[1], xs[3])
    for partner in near:
        pl.semaphore_signal(barrier, inc=1, device_id=partner, device_id_type=MESH)
    for copy in loads:
        copy.start()
    first = span_ref[0].astype(f32)
    second = span_ref[1].astype(f32)
    lane = lax.broadcasted_iota(jnp.int32, (16, 128), 1)
    row = lax.broadcasted_iota(jnp.int32, (16, 128), 0)
    kbuf[0, WIDTH:KROWS, :] = jnp.where(lane < SPAN, first, second).astype(bf16)
    qpos[0] = jnp.where(row < 8, first, second).astype(bf16)
    kt[:, QK:DEEP, :] = jnp.zeros((HEADS_DEV, DEEP - QK, 16 * ROWS), bf16)
    loads[0].wait()
    pl.semaphore_wait(barrier, len(near))

    def send(src, dst, kind, r_sem, device):
        pltpu.make_async_remote_copy(
            src_ref=src, dst_ref=dst, send_sem=send_sem.at[kind], recv_sem=r_sem,
            device_id=device, device_id_type=MESH,
        ).start()

    def arrived(ref, sem):
        pltpu.make_async_copy(ref, ref, sem).wait()

    def piece(slot, p):
        begin, size = PIECES[p]
        return kbuf.at[slot, pl.ds(begin, size)]

    def send_k(slot, p, there, device):
        send(piece(slot, p), piece(there, p), 0, kr_sem.at[KEY_SEM[there, p]], device)

    def to_sib(slot):
        send(kbuf.at[slot], kbuf.at[slot + 4], 0, kr_sem.at[KEY_SEM[slot + 4, 0]], sib)

    def wait_k(slot, p=None):
        if p is None:
            arrived(kbuf.at[slot], kr_sem.at[KEY_SEM[slot, 0]])
        else:
            arrived(piece(slot, p), kr_sem.at[KEY_SEM[slot, p]])

    def qpart(slot, b):
        return qx.at[slot, pl.ds(b * SPAN, SPAN)]

    def send_q(slot, b, there, device):
        send(qpart(slot, b), qpart(there, b), 1, qr_sem.at[there - 1, b], device)

    def wait_q(slot, b):
        arrived(qpart(slot, b), qr_sem.at[slot - 1, b])

    def send_pos(slot, there, device):
        send(qpos.at[slot], qpos.at[there], 2, pr_sem.at[there - 1], device)

    def wait_pos(slot):
        arrived(qpos.at[slot], pr_sem.at[slot - 1])

    for p in range(HALF):
        send_k(0, p, 3, yp)
        send_k(0, p + HALF, 1, ym)
        send_k(0, p, 8, zp)
        send_k(0, p + HALF, 8, zm)
    to_sib(0)
    send_pos(0, 3, xs[1])
    send_pos(0, 1, xs[3])
    loads[1].wait()
    loads[2].wait()
    send_q(0, 0, 3, xs[1])
    send_q(0, 1, 1, xs[3])
    for p in range(HALF):
        send_k(0, p + HALF, 3, yp)
        send_k(0, p, 1, ym)
    send_q(0, 1, 3, xs[1])
    send_q(0, 0, 1, xs[3])

    column = lax.broadcasted_iota(jnp.int32, (ROWS, ROPE), 1)
    late = lax.broadcasted_iota(jnp.int32, (ROWS, ROPE), 0) // SPAN

    def build_q(k):
        d = ARRIVAL[k]
        for head in range(HEADS_DEV):
            qs[head, k, :, 0:NOPE] = qx[d, :, head * NOPE : (head + 1) * NOPE]
            begin = HEADS_DEV * NOPE + head * ROPE
            qs[head, k, :, NOPE:QK] = qx[d, :, begin : begin + ROPE]
            qs[head, k, :, QK:DEEP] = jnp.where(column == 2 * k + late, 1.0, 0.0).astype(bf16)
        spans = qpos[d].astype(f32)
        qspan[2 * k : 2 * k + 1, :] = spans[0:1, :]
        qspan[2 * k + 1 : 2 * k + 2, :] = spans[8:9, :]

    def columns(chunk):
        return slice(STARTS[chunk], STARTS[chunk] + ROWS * len(CHUNKS[chunk]))

    def later(chunk, first=0, count=4):
        for j, slot in enumerate(CHUNKS[chunk]):
            if not first <= j < first + count:
                continue
            begin = STARTS[chunk] + j * ROWS
            span = kbuf[slot, WIDTH:KROWS, :].astype(f32)[0:8, :]
            bias = jnp.where(span > qspan[...], LOWEST, 0.0)
            bias = jnp.concatenate([bias, jnp.zeros((8, 128), f32)], axis=0).astype(bf16)
            for head in range(HEADS_DEV):
                kt[head, QK : QK + 16, begin : begin + ROWS] = bias

    def lift(chunk, first=0, count=4):
        slots = CHUNKS[chunk][first : first + count]
        begin = STARTS[chunk] + first * ROWS
        where = slice(begin, begin + len(slots) * ROWS)
        latents = jnp.concatenate([kbuf[s, 0:LATENT, :] for s in slots], axis=1)
        keys = lax.dot_general(wk[...], latents, NN, preferred_element_type=f32).astype(bf16)
        ropes = jnp.concatenate([kbuf[s, LATENT:WIDTH, :] for s in slots], axis=1)
        for head in range(HEADS_DEV):
            kt[head, 0:NOPE, where] = keys[head * NOPE : (head + 1) * NOPE]
            kt[head, NOPE:QK, where] = ropes
        v_sc[where, :] = lax.dot_general(
            latents, vu[...], (((0,), (0,)), ((), ())), preferred_element_type=f32
        ).astype(bf16)
        later(chunk, first, count)

    rowid = lax.broadcasted_iota(jnp.int32, (ROWS, ROWS), 0)
    keyid = lax.broadcasted_iota(jnp.int32, (ROWS, ROWS), 1)
    ahead = (keyid > rowid) & (keyid // SPAN == rowid // SPAN)

    def scores(chunk, low, high):
        count = (high - low) * ROWS
        size = len(CHUNKS[chunk])
        for head in range(HEADS_DEV):
            values = lax.dot_general(
                qs[head, low:high].reshape(count, DEEP), kt[head, :, columns(chunk)], NN,
                preferred_element_type=f32,
            )
            peak = m_sc[head, low:high].reshape(count, 128) if chunk else None
            for j in range(size):
                part = values[:, j * 128 : (j + 1) * 128] * SCALE
                if chunk == 0 and low == 0 and j == 0:
                    part = jnp.where(ahead, LOWEST, part)
                begin = STARTS[chunk] + j * 128
                s_sc[head, low:high, :, begin : begin + 128] = part.reshape(high - low, ROWS, 128)
                peak = part if peak is None else jnp.maximum(peak, part)
            m_sc[head, low:high] = peak.reshape(high - low, ROWS, 128)

    build_q(0)
    loads[3].wait()
    wk[...] = jnp.transpose(ku[...])
    loads[4].wait()
    wait_k(4)
    lift(0)
    scores(0, 0, 1)
    for p in range(HALF):
        wait_k(3, p)
        send_k(3, p, 2, yp)
        send_k(3, p, 11, zp)
        wait_k(1, p + HALF)
        send_k(1, p + HALF, 2, ym)
        send_k(1, p + HALF, 9, zm)
    for p in range(HALF):
        wait_k(8, p)
        send_k(8, p, 9, ym)
        wait_k(8, p + HALF)
        send_k(8, p + HALF, 11, yp)
    to_sib(8)
    wait_q(3, 0)
    send_q(3, 0, 2, xs[1])
    wait_q(1, 1)
    send_q(1, 1, 2, xs[3])
    wait_pos(3)
    send_pos(3, 2, xs[1])
    wait_pos(1)
    for p in range(HALF):
        wait_k(3, p + HALF)
        wait_k(1, p)
    to_sib(3)
    to_sib(1)
    wait_k(12)
    lift(1)
    scores(1, 0, 1)
    for p in range(HALF):
        wait_k(2, p)
        send_k(2, p, 10, zp)
        wait_k(2, p + HALF)
        send_k(2, p + HALF, 10, zm)
    to_sib(2)
    wait_q(3, 1)
    build_q(1)
    wait_q(1, 0)
    build_q(2)
    later(0)
    later(1)
    scores(0, 1, 3)
    scores(1, 1, 3)
    wait_k(5)
    wait_k(7)
    lift(2)
    scores(2, 0, 3)
    for slot in (11, 9):
        for p in range(2 * HALF):
            wait_k(slot, p)
        to_sib(slot)
    for b in (0, 1):
        wait_q(2, b)
    wait_pos(2)
    build_q(3)
    for chunk in range(3):
        later(chunk)
    scores(0, 3, 4)
    scores(1, 3, 4)
    scores(2, 3, 4)
    wait_k(6)
    lift(3)
    for p in range(2 * HALF):
        wait_k(10, p)
    to_sib(10)
    scores(3, 0, 4)
    wait_k(13)
    wait_k(15)
    lift(LAST, 0, 2)
    wait_k(14)
    lift(LAST, 2, 2)

    def weigh(r):
        begin, size = PARTS[r]
        rows = slice(begin, begin + size)
        count = 4 * size
        heads = range(HEADS_DEV)
        scored = [
            lax.dot_general(
                qs[head, :, rows, :].reshape(count, DEEP), kt[head, :, columns(LAST)], NN,
                preferred_element_type=f32,
            )
            for head in heads
        ]
        kept = STARTS[LAST] // 128
        fresh, peaks = [], []
        for head in heads:
            peak = m_sc[head, :, rows, :].reshape(count, 128)
            parts = []
            for j in range(len(CHUNKS[LAST])):
                parts.append(scored[head][:, j * 128 : (j + 1) * 128] * SCALE)
                peak = jnp.maximum(peak, parts[-1])
            fresh.append(parts)
            peaks.append(jnp.broadcast_to(jnp.max(peak, axis=1, keepdims=True), (count, 128)))
        results = []
        for head in heads:
            total = None
            ws = []
            for n in range(16):
                if n < kept:
                    part = s_sc[head, :, rows, n * 128 : (n + 1) * 128].reshape(count, 128)
                else:
                    part = fresh[head][n - kept]
                w = jnp.exp2(part - peaks[head])
                total = w if total is None else total + w
                ws.append(w.astype(bf16))
            out = lax.dot_general(
                jnp.concatenate(ws, axis=1), v_sc[:, head * 128 : (head + 1) * 128], NN,
                preferred_element_type=f32,
            )
            results.append((peaks[head], total, out))
        denoms = [jnp.sum(total, axis=1, keepdims=True) for _, total, _ in results]
        for head, (peak, _, out) in enumerate(results):
            part = (out * (1.0 / denoms[head])).astype(bf16)
            for k, d in enumerate(ARRIVAL):
                pbuf[d, rows, head * 128 : (head + 1) * 128] = part[k * size : (k + 1) * size]
            log = peak + jnp.broadcast_to(jnp.log(denoms[head]) * LOG2E, (4 * size, 128))
            log = jnp.concatenate([log] * (32 // size), axis=0)
            stat[r, head : head + 1, :] = jnp.transpose(log)[0:1, :]
        here = pl.ds(begin, size)
        for d in (2, 1, 3):
            send(pbuf.at[d, here], rbuf.at[d - 1, here], 3, rr_sem.at[r], xs[d])
            send(stat.at[r], rstat.at[r, d - 1], 4, tr_sem.at[r], xs[d])

    def merge(r):
        begin, size = PARTS[r]
        rows, here = slice(begin, begin + size), pl.ds(begin, size)
        arrived(rstat.at[r], tr_sem.at[r])
        arrived(rbuf.at[:, here], rr_sem.at[r])
        tiles = [stat[r]] + [rstat[r, d] for d in range(3)]
        tops = []
        for d, tile in enumerate(tiles):
            k = ARRIVAL.index(d)
            tops.append(jnp.transpose(jnp.concatenate([tile, tile], axis=0))[k * size : (k + 1) * size, :])
        heads = []
        for head in range(HEADS_DEV):
            logs = [col[:, head : head + 1] for col in tops]
            top = jnp.maximum(jnp.maximum(logs[0], logs[1]), jnp.maximum(logs[2], logs[3]))
            scale = [jnp.exp2(v - top) for v in logs]
            total = scale[0] + scale[1] + scale[2] + scale[3]
            where = slice(head * 128, (head + 1) * 128)
            acc = pbuf[0, rows, where].astype(f32) * scale[0]
            for d in range(3):
                acc = acc + rbuf[d, rows, where].astype(f32) * scale[d + 1]
            heads.append((acc * (1.0 / total)).astype(bf16))
        head_out = jnp.concatenate(heads, axis=1)
        low, high = pl.ds(0, 256), pl.ds(256, 256)
        mixed = []
        for d in (2, 1, 3, 0):
            start = pl.multiple_of(((h + d) % 4) * 512, 512)
            mixed.append(lax.dot_general(
                head_out, op[:, pl.ds(start, 512)], NN, preferred_element_type=f32
            ).astype(bf16))
        for d, y in zip((2, 1, 3, 0), mixed):
            ybuf[d, rows] = y
        if r == R - 1:
            send(ybuf.at[2, here], y3, 7, zr_sem.at[r, 0], far)
            send(ybuf.at[1, here], y2.at[0, here], 6, zr_sem.at[r, 2], hp)
            send(ybuf.at[3, here], y2.at[1, here], 6, zr_sem.at[r, 2], hm)
            return
        send(ybuf.at[2, here, low], y1.at[0, here], 5, zr_sem.at[r, 0], hp)
        send(ybuf.at[2, here, high], y1.at[1, here], 5, zr_sem.at[r, 1], hm)
        send(ybuf.at[1, here, high], y2.at[0, here, high], 6, zr_sem.at[r, 2], hp)
        send(ybuf.at[3, here, low], y2.at[1, here, low], 6, zr_sem.at[r, 2], hm)

    def pass_on(r):
        begin, size = PARTS[r]
        rows, here = slice(begin, begin + size), pl.ds(begin, size)
        low, high = pl.ds(0, 256), pl.ds(256, 256)
        arrived(y1.at[0, here], zr_sem.at[r, 0])
        left = ybuf[1, rows, 0:256].astype(f32) + y1[0, rows].astype(f32)
        ysum[0, rows] = left.astype(bf16)
        send(ysum.at[0, here], y2.at[0, here, low], 6, zr_sem.at[r, 2], hp)
        arrived(y1.at[1, here], zr_sem.at[r, 1])
        right = ybuf[3, rows, 256:512].astype(f32) + y1[1, rows].astype(f32)
        ysum[1, rows] = right.astype(bf16)
        send(ysum.at[1, here], y2.at[1, here, high], 6, zr_sem.at[r, 2], hm)

    def finish(r):
        begin, size = PARTS[r]
        rows, here = slice(begin, begin + size), pl.ds(begin, size)
        arrived(y2.at[:, here], zr_sem.at[r, 2])
        total = ybuf[0, rows].astype(f32) + y2[0, rows].astype(f32) + y2[1, rows].astype(f32)
        if r == R - 1:
            arrived(y3, zr_sem.at[r, 0])
            total = total + y3[...].astype(f32)
        out_ref[rows, :] = total.astype(bf16)

    weigh(0)
    weigh(1)
    weigh(2)
    weigh(3)
    weigh(4)
    loads[5].wait()
    merge(0)
    merge(1)
    merge(2)
    pass_on(0)
    merge(3)
    pass_on(1)
    merge(4)
    pass_on(2)
    pass_on(3)
    for r in range(R):
        finish(r)
    for kind, ref in enumerate((
        kbuf.at[pl.ds(0, 15)], qx.at[pl.ds(0, 3)], qpos.at[pl.ds(0, 3)], rbuf, rstat,
        y1.at[:, pl.ds(0, PARTS[-1][0])], y2, y3,
    )):
        arrived(ref, send_sem.at[kind])


def shards(query_nope, query_rope, cache, span_ids, key_up, value_up, out_proj):
    anywhere = pl.BlockSpec(memory_space=pl.ANY)
    dma = pltpu.SemaphoreType.DMA
    return pl.pallas_call(
        kernel,
        name="attend",
        out_shape=jax.ShapeDtypeStruct((ROWS, 512), bf16),
        in_specs=[pl.BlockSpec(memory_space=pltpu.SMEM)] + [anywhere] * 6,
        out_specs=pl.BlockSpec(memory_space=pltpu.VMEM),
        scratch_shapes=[
            pltpu.VMEM((16, KROWS, ROWS), bf16),
            pltpu.VMEM((4, ROWS, QWIDTH), bf16),
            pltpu.VMEM((4, 16, 128), bf16),
            pltpu.VMEM((512, 512), bf16),
            pltpu.VMEM((512, 512), bf16),
            pltpu.VMEM((512, 2048), bf16),
            pltpu.VMEM((512, LATENT), bf16),
            pltpu.VMEM((HEADS_DEV, DEEP, 16 * ROWS), bf16),
            pltpu.VMEM((16 * ROWS, 512), bf16),
            pltpu.VMEM((HEADS_DEV, 4, ROWS, DEEP), bf16),
            pltpu.VMEM((8, 128), f32),
            pltpu.VMEM((HEADS_DEV, 4, ROWS, 16 * ROWS), f32),
            pltpu.VMEM((HEADS_DEV, 4, ROWS, 128), f32),
            pltpu.VMEM((4, ROWS, 512), bf16),
            pltpu.VMEM((R, 4, 128), f32),
            pltpu.VMEM((3, ROWS, 512), bf16),
            pltpu.VMEM((R, 3, 4, 128), f32),
            pltpu.VMEM((4, ROWS, 512), bf16),
            pltpu.VMEM((2, ROWS, 256), bf16),
            pltpu.VMEM((2, ROWS, 256), bf16),
            pltpu.VMEM((2, ROWS, 512), bf16),
            pltpu.VMEM((PARTS[-1][1], 512), bf16),
            dma((6,)),
            dma((len(set(KEY_SEM.values())),)),
            dma((3, 2)),
            dma((3,)),
            dma((R,)),
            dma((R,)),
            dma((R, 3)),
            dma((8,)),
        ],
        compiler_params=pltpu.CompilerParams(
            collective_id=0, has_side_effects=True, vmem_limit_bytes=48 * 2**20
        ),
    )(*(
        pltpu.with_memory_space_constraint(a, pltpu.HBM)
        for a in (span_ids, query_nope, query_rope, cache.T, key_up, value_up, out_proj)
    ))


def solution(mesh):
    rows = ("outer", "inner")
    return jax.shard_map(
        shards,
        mesh=mesh,
        in_specs=(
            P(rows, "head"),
            P(rows, "head"),
            P(rows, None),
            P(rows),
            P(None, "head"),
            P(None, "head"),
            P("head", None),
        ),
        out_specs=P(rows, "head"),
        check_vma=False,
    )
```

```python
import jax
import jax.numpy as jnp
from jax import lax
from jax.experimental import pallas as pl
from jax.experimental.pallas import tpu as pltpu
from jax.sharding import PartitionSpec as P

LATENT = 512
ROPE = 64
NOPE = 128
SPAN = 64
HEADS_DEV = 4
ROWS = 128
WIDTH = LATENT + ROPE
QK = NOPE + ROPE
QWIDTH = HEADS_DEV * (NOPE + ROPE)
PARTS = ((0, 16), (16, 32), (48, 32), (80, 32), (112, 16))
R = len(PARTS)
DEEP = 256
KROWS = WIDTH + 16
PIECES = ((0, 96), (96, 96), (192, 96), (288, 96), (384, 96), (480, 112))
HALF = 3
SCALE = (NOPE + ROPE) ** -0.5 * 1.4426950408889634
LOG2E = 1.4426950408889634
LOWEST = -1e30
ARRIVAL = (0, 3, 1, 2)
MESH = pl.DeviceIdType.MESH
NN = (((1,), (0,)), ((), ()))
f32 = jnp.float32
bf16 = jnp.bfloat16
BOTH = (4, 5, 6, 7, 9, 10, 11, 12, 13, 14, 15)
KEY_SEM = {}
for _slot in range(1, 16):
    for _p in range(2 * HALF):
        if _slot in BOTH and _p:
            KEY_SEM[_slot, _p] = KEY_SEM[_slot, 0]
        else:
            KEY_SEM[_slot, _p] = len(set(KEY_SEM.values()))
CHUNKS = ((0, 4), (8, 12), (1, 5, 3, 7), (2, 6, 9, 11), (13, 15, 10, 14))
STARTS = (0, 256, 512, 1024, 1536)
LAST = len(CHUNKS) - 1


def kernel(
    span_ref, qn_ref, qr_ref, k_ref, ku_ref, vu_ref, op_ref, out_ref,
    kbuf, qx, qpos, ku, vu, op, wk, kt, v_sc, qs, qspan, s_sc, m_sc, pbuf, stat, rbuf, rstat,
    ybuf, y1, ysum, y2, y3,
    load_sem, kr_sem, qr_sem, pr_sem, rr_sem, tr_sem, zr_sem, send_sem,
):
    h = lax.axis_index("head")
    o = lax.axis_index("outer")
    i = lax.axis_index("inner")
    zl, c = o // 2, o % 2
    y, x = i // 4, i % 4
    z = h * 2 + zl

    def at_z(zz):
        return (zz // 2, (zz % 2) * 2 + c, i)

    sib = (h, zl * 2 + 1 - c, i)
    yp = (h, o, ((y + 1) % 4) * 4 + x)
    ym = (h, o, ((y + 3) % 4) * 4 + x)
    zp = at_z((z + 1) % 8)
    zm = at_z((z + 7) % 8)
    xs = [None] + [(h, o, y * 4 + (x + d) % 4) for d in (1, 2, 3)]
    hp = ((h + 1) % 4, o, i)
    hm = ((h + 3) % 4, o, i)
    far = ((h + 2) % 4, o, i)

    loads = [
        pltpu.make_async_copy(k_ref, kbuf.at[0, pl.ds(0, WIDTH)], load_sem.at[0]),
        pltpu.make_async_copy(qn_ref, qx.at[0, :, pl.ds(0, 512)], load_sem.at[1]),
        pltpu.make_async_copy(qr_ref, qx.at[0, :, pl.ds(512, 256)], load_sem.at[2]),
        pltpu.make_async_copy(ku_ref, ku, load_sem.at[3]),
        pltpu.make_async_copy(vu_ref, vu, load_sem.at[4]),
        pltpu.make_async_copy(op_ref, op, load_sem.at[5]),
    ]
    barrier = pltpu.get_barrier_semaphore()
    near = (sib, yp, ym, zp, zm, xs[1], xs[3])
    for partner in near:
        pl.semaphore_signal(barrier, inc=1, device_id=partner, device_id_type=MESH)
    for copy in loads:
        copy.start()
    first = span_ref[0].astype(f32)
    second = span_ref[1].astype(f32)
    lane = lax.broadcasted_iota(jnp.int32, (16, 128), 1)
    row = lax.broadcasted_iota(jnp.int32, (16, 128), 0)
    kbuf[0, WIDTH:KROWS, :] = jnp.where(lane < SPAN, first, second).astype(bf16)
    qpos[0] = jnp.where(row < 8, first, second).astype(bf16)
    kt[:, QK:DEEP, :] = jnp.zeros((HEADS_DEV, DEEP - QK, 16 * ROWS), bf16)
    loads[0].wait()
    pl.semaphore_wait(barrier, len(near))

    def send(src, dst, kind, r_sem, device):
        pltpu.make_async_remote_copy(
            src_ref=src, dst_ref=dst, send_sem=send_sem.at[kind], recv_sem=r_sem,
            device_id=device, device_id_type=MESH,
        ).start()

    def arrived(ref, sem):
        pltpu.make_async_copy(ref, ref, sem).wait()

    def piece(slot, p):
        begin, size = PIECES[p]
        return kbuf.at[slot, pl.ds(begin, size)]

    def send_k(slot, p, there, device):
        send(piece(slot, p), piece(there, p), 0, kr_sem.at[KEY_SEM[there, p]], device)

    def to_sib(slot):
        send(kbuf.at[slot], kbuf.at[slot + 4], 0, kr_sem.at[KEY_SEM[slot + 4, 0]], sib)

    def wait_k(slot, p=None):
        if p is None:
            arrived(kbuf.at[slot], kr_sem.at[KEY_SEM[slot, 0]])
        else:
            arrived(piece(slot, p), kr_sem.at[KEY_SEM[slot, p]])

    def qpart(slot, b):
        return qx.at[slot, pl.ds(b * SPAN, SPAN)]

    def send_q(slot, b, there, device):
        send(qpart(slot, b), qpart(there, b), 1, qr_sem.at[there - 1, b], device)

    def wait_q(slot, b):
        arrived(qpart(slot, b), qr_sem.at[slot - 1, b])

    def send_pos(slot, there, device):
        send(qpos.at[slot], qpos.at[there], 2, pr_sem.at[there - 1], device)

    def wait_pos(slot):
        arrived(qpos.at[slot], pr_sem.at[slot - 1])

    for p in range(HALF):
        send_k(0, p, 3, yp)
        send_k(0, p + HALF, 1, ym)
        send_k(0, p, 8, zp)
        send_k(0, p + HALF, 8, zm)
    to_sib(0)
    send_pos(0, 3, xs[1])
    send_pos(0, 1, xs[3])
    loads[1].wait()
    loads[2].wait()
    send_q(0, 0, 3, xs[1])
    send_q(0, 1, 1, xs[3])
    for p in range(HALF):
        send_k(0, p + HALF, 3, yp)
        send_k(0, p, 1, ym)
    send_q(0, 1, 3, xs[1])
    send_q(0, 0, 1, xs[3])

    column = lax.broadcasted_iota(jnp.int32, (ROWS, ROPE), 1)
    late = lax.broadcasted_iota(jnp.int32, (ROWS, ROPE), 0) // SPAN

    def build_q(k):
        d = ARRIVAL[k]
        for head in range(HEADS_DEV):
            qs[head, k, :, 0:NOPE] = qx[d, :, head * NOPE : (head + 1) * NOPE]
            begin = HEADS_DEV * NOPE + head * ROPE
            qs[head, k, :, NOPE:QK] = qx[d, :, begin : begin + ROPE]
            qs[head, k, :, QK:DEEP] = jnp.where(column == 2 * k + late, 1.0, 0.0).astype(bf16)
        spans = qpos[d].astype(f32)
        qspan[2 * k : 2 * k + 1, :] = spans[0:1, :]
        qspan[2 * k + 1 : 2 * k + 2, :] = spans[8:9, :]

    def columns(chunk):
        return slice(STARTS[chunk], STARTS[chunk] + ROWS * len(CHUNKS[chunk]))

    def later(chunk, first=0, count=4):
        for j, slot in enumerate(CHUNKS[chunk]):
            if not first <= j < first + count:
                continue
            begin = STARTS[chunk] + j * ROWS
            span = kbuf[slot, WIDTH:KROWS, :].astype(f32)[0:8, :]
            bias = jnp.where(span > qspan[...], LOWEST, 0.0)
            bias = jnp.concatenate([bias, jnp.zeros((8, 128), f32)], axis=0).astype(bf16)
            for head in range(HEADS_DEV):
                kt[head, QK : QK + 16, begin : begin + ROWS] = bias

    def lift(chunk, first=0, count=4):
        slots = CHUNKS[chunk][first : first + count]
        begin = STARTS[chunk] + first * ROWS
        where = slice(begin, begin + len(slots) * ROWS)
        latents = jnp.concatenate([kbuf[s, 0:LATENT, :] for s in slots], axis=1)
        keys = lax.dot_general(wk[...], latents, NN, preferred_element_type=f32).astype(bf16)
        ropes = jnp.concatenate([kbuf[s, LATENT:WIDTH, :] for s in slots], axis=1)
        for head in range(HEADS_DEV):
            kt[head, 0:NOPE, where] = keys[head * NOPE : (head + 1) * NOPE]
            kt[head, NOPE:QK, where] = ropes
        v_sc[where, :] = lax.dot_general(
            latents, vu[...], (((0,), (0,)), ((), ())), preferred_element_type=f32
        ).astype(bf16)
        later(chunk, first, count)

    rowid = lax.broadcasted_iota(jnp.int32, (ROWS, ROWS), 0)
    keyid = lax.broadcasted_iota(jnp.int32, (ROWS, ROWS), 1)
    ahead = (keyid > rowid) & (keyid // SPAN == rowid // SPAN)

    def scores(chunk, low, high):
        count = (high - low) * ROWS
        size = len(CHUNKS[chunk])
        for head in range(HEADS_DEV):
            values = lax.dot_general(
                qs[head, low:high].reshape(count, DEEP), kt[head, :, columns(chunk)], NN,
                preferred_element_type=f32,
            )
            peak = m_sc[head, low:high].reshape(count, 128) if chunk else None
            for j in range(size):
                part = values[:, j * 128 : (j + 1) * 128] * SCALE
                if chunk == 0 and low == 0 and j == 0:
                    part = jnp.where(ahead, LOWEST, part)
                begin = STARTS[chunk] + j * 128
                s_sc[head, low:high, :, begin : begin + 128] = part.reshape(high - low, ROWS, 128)
                peak = part if peak is None else jnp.maximum(peak, part)
            m_sc[head, low:high] = peak.reshape(high - low, ROWS, 128)

    build_q(0)
    loads[3].wait()
    wk[...] = jnp.transpose(ku[...])
    loads[4].wait()
    wait_k(4)
    lift(0)
    scores(0, 0, 1)
    for p in range(HALF):
        wait_k(3, p)
        send_k(3, p, 2, yp)
        send_k(3, p, 11, zp)
        wait_k(1, p + HALF)
        send_k(1, p + HALF, 2, ym)
        send_k(1, p + HALF, 9, zm)
    for p in range(HALF):
        wait_k(8, p)
        send_k(8, p, 9, ym)
        wait_k(8, p + HALF)
        send_k(8, p + HALF, 11, yp)
    to_sib(8)
    wait_q(3, 0)
    send_q(3, 0, 2, xs[1])
    wait_q(1, 1)
    send_q(1, 1, 2, xs[3])
    wait_pos(3)
    send_pos(3, 2, xs[1])
    wait_pos(1)
    for p in range(HALF):
        wait_k(3, p + HALF)
        wait_k(1, p)
    to_sib(3)
    to_sib(1)
    wait_k(12)
    lift(1)
    scores(1, 0, 1)
    for p in range(HALF):
        wait_k(2, p)
        send_k(2, p, 10, zp)
        wait_k(2, p + HALF)
        send_k(2, p + HALF, 10, zm)
    to_sib(2)
    wait_q(3, 1)
    build_q(1)
    wait_q(1, 0)
    build_q(2)
    later(0)
    later(1)
    scores(0, 1, 3)
    scores(1, 1, 3)
    wait_k(5)
    wait_k(7)
    lift(2)
    scores(2, 0, 3)
    for slot in (11, 9):
        wait_k(slot)
        to_sib(slot)
    for b in (0, 1):
        wait_q(2, b)
    wait_pos(2)
    build_q(3)
    for chunk in range(3):
        later(chunk)
    scores(0, 3, 4)
    scores(1, 3, 4)
    scores(2, 3, 4)
    wait_k(6)
    lift(3)
    wait_k(10)
    to_sib(10)
    scores(3, 0, 4)
    wait_k(13)
    wait_k(15)
    lift(LAST, 0, 2)
    wait_k(14)
    lift(LAST, 2, 2)

    def weigh(r):
        begin, size = PARTS[r]
        rows = slice(begin, begin + size)
        count = 4 * size
        heads = range(HEADS_DEV)
        scored = [
            lax.dot_general(
                qs[head, :, rows, :].reshape(count, DEEP), kt[head, :, columns(LAST)], NN,
                preferred_element_type=f32,
            )
            for head in heads
        ]
        kept = STARTS[LAST] // 128
        fresh, peaks = [], []
        for head in heads:
            peak = m_sc[head, :, rows, :].reshape(count, 128)
            parts = []
            for j in range(len(CHUNKS[LAST])):
                parts.append(scored[head][:, j * 128 : (j + 1) * 128] * SCALE)
                peak = jnp.maximum(peak, parts[-1])
            fresh.append(parts)
            peaks.append(jnp.broadcast_to(jnp.max(peak, axis=1, keepdims=True), (count, 128)))
        results = []
        for head in heads:
            total = None
            ws = []
            for n in range(16):
                if n < kept:
                    part = s_sc[head, :, rows, n * 128 : (n + 1) * 128].reshape(count, 128)
                else:
                    part = fresh[head][n - kept]
                w = jnp.exp2(part - peaks[head])
                total = w if total is None else total + w
                ws.append(w.astype(bf16))
            out = lax.dot_general(
                jnp.concatenate(ws, axis=1), v_sc[:, head * 128 : (head + 1) * 128], NN,
                preferred_element_type=f32,
            )
            results.append((peaks[head], total, out))
        denoms = [jnp.sum(total, axis=1, keepdims=True) for _, total, _ in results]
        for head, (peak, _, out) in enumerate(results):
            part = (out * (1.0 / denoms[head])).astype(bf16)
            for k, d in enumerate(ARRIVAL):
                pbuf[d, rows, head * 128 : (head + 1) * 128] = part[k * size : (k + 1) * size]
            log = peak + jnp.broadcast_to(jnp.log(denoms[head]) * LOG2E, (4 * size, 128))
            log = jnp.concatenate([log] * (32 // size), axis=0)
            stat[r, head : head + 1, :] = jnp.transpose(log)[0:1, :]
        here = pl.ds(begin, size)
        for d in (2, 1, 3):
            send(pbuf.at[d, here], rbuf.at[d - 1, here], 3, rr_sem.at[r], xs[d])
            send(stat.at[r], rstat.at[r, d - 1], 4, tr_sem.at[r], xs[d])

    def merge(r):
        begin, size = PARTS[r]
        rows, here = slice(begin, begin + size), pl.ds(begin, size)
        arrived(rstat.at[r], tr_sem.at[r])
        arrived(rbuf.at[:, here], rr_sem.at[r])
        tiles = [stat[r]] + [rstat[r, d] for d in range(3)]
        tops = []
        for d, tile in enumerate(tiles):
            k = ARRIVAL.index(d)
            tops.append(jnp.transpose(jnp.concatenate([tile, tile], axis=0))[k * size : (k + 1) * size, :])
        heads = []
        for head in range(HEADS_DEV):
            logs = [col[:, head : head + 1] for col in tops]
            top = jnp.maximum(jnp.maximum(logs[0], logs[1]), jnp.maximum(logs[2], logs[3]))
            scale = [jnp.exp2(v - top) for v in logs]
            total = scale[0] + scale[1] + scale[2] + scale[3]
            where = slice(head * 128, (head + 1) * 128)
            acc = pbuf[0, rows, where].astype(f32) * scale[0]
            for d in range(3):
                acc = acc + rbuf[d, rows, where].astype(f32) * scale[d + 1]
            heads.append((acc * (1.0 / total)).astype(bf16))
        head_out = jnp.concatenate(heads, axis=1)
        low, high = pl.ds(0, 256), pl.ds(256, 256)
        mixed = []
        for d in (2, 1, 3, 0):
            start = pl.multiple_of(((h + d) % 4) * 512, 512)
            mixed.append(lax.dot_general(
                head_out, op[:, pl.ds(start, 512)], NN, preferred_element_type=f32
            ).astype(bf16))
        for d, y in zip((2, 1, 3, 0), mixed):
            ybuf[d, rows] = y
        if r == R - 1:
            send(ybuf.at[2, here], y3, 7, zr_sem.at[r, 0], far)
            send(ybuf.at[1, here], y2.at[0, here], 6, zr_sem.at[r, 2], hp)
            send(ybuf.at[3, here], y2.at[1, here], 6, zr_sem.at[r, 2], hm)
            return
        send(ybuf.at[2, here, low], y1.at[0, here], 5, zr_sem.at[r, 0], hp)
        send(ybuf.at[2, here, high], y1.at[1, here], 5, zr_sem.at[r, 1], hm)
        send(ybuf.at[1, here, high], y2.at[0, here, high], 6, zr_sem.at[r, 2], hp)
        send(ybuf.at[3, here, low], y2.at[1, here, low], 6, zr_sem.at[r, 2], hm)

    def pass_on(r):
        begin, size = PARTS[r]
        rows, here = slice(begin, begin + size), pl.ds(begin, size)
        low, high = pl.ds(0, 256), pl.ds(256, 256)
        arrived(y1.at[0, here], zr_sem.at[r, 0])
        left = ybuf[1, rows, 0:256].astype(f32) + y1[0, rows].astype(f32)
        ysum[0, rows] = left.astype(bf16)
        send(ysum.at[0, here], y2.at[0, here, low], 6, zr_sem.at[r, 2], hp)
        arrived(y1.at[1, here], zr_sem.at[r, 1])
        right = ybuf[3, rows, 256:512].astype(f32) + y1[1, rows].astype(f32)
        ysum[1, rows] = right.astype(bf16)
        send(ysum.at[1, here], y2.at[1, here, high], 6, zr_sem.at[r, 2], hm)

    def finish(r):
        begin, size = PARTS[r]
        rows, here = slice(begin, begin + size), pl.ds(begin, size)
        arrived(y2.at[:, here], zr_sem.at[r, 2])
        total = ybuf[0, rows].astype(f32) + y2[0, rows].astype(f32) + y2[1, rows].astype(f32)
        if r == R - 1:
            arrived(y3, zr_sem.at[r, 0])
            total = total + y3[...].astype(f32)
        out_ref[rows, :] = total.astype(bf16)

    weigh(0)
    weigh(1)
    weigh(2)
    weigh(3)
    weigh(4)
    loads[5].wait()
    merge(0)
    merge(1)
    merge(2)
    pass_on(0)
    merge(3)
    pass_on(1)
    merge(4)
    pass_on(2)
    pass_on(3)
    for r in range(R):
        finish(r)
    for kind, ref in enumerate((
        kbuf.at[pl.ds(0, 15)], qx.at[pl.ds(0, 3)], qpos.at[pl.ds(0, 3)], rbuf, rstat,
        y1.at[:, pl.ds(0, PARTS[-1][0])], y2, y3,
    )):
        arrived(ref, send_sem.at[kind])


def shards(query_nope, query_rope, cache, span_ids, key_up, value_up, out_proj):
    anywhere = pl.BlockSpec(memory_space=pl.ANY)
    dma = pltpu.SemaphoreType.DMA
    return pl.pallas_call(
        kernel,
        name="attend",
        out_shape=jax.ShapeDtypeStruct((ROWS, 512), bf16),
        in_specs=[pl.BlockSpec(memory_space=pltpu.SMEM)] + [anywhere] * 6,
        out_specs=pl.BlockSpec(memory_space=pltpu.VMEM),
        scratch_shapes=[
            pltpu.VMEM((16, KROWS, ROWS), bf16),
            pltpu.VMEM((4, ROWS, QWIDTH), bf16),
            pltpu.VMEM((4, 16, 128), bf16),
            pltpu.VMEM((512, 512), bf16),
            pltpu.VMEM((512, 512), bf16),
            pltpu.VMEM((512, 2048), bf16),
            pltpu.VMEM((512, LATENT), bf16),
            pltpu.VMEM((HEADS_DEV, DEEP, 16 * ROWS), bf16),
            pltpu.VMEM((16 * ROWS, 512), bf16),
            pltpu.VMEM((HEADS_DEV, 4, ROWS, DEEP), bf16),
            pltpu.VMEM((8, 128), f32),
            pltpu.VMEM((HEADS_DEV, 4, ROWS, 16 * ROWS), f32),
            pltpu.VMEM((HEADS_DEV, 4, ROWS, 128), f32),
            pltpu.VMEM((4, ROWS, 512), bf16),
            pltpu.VMEM((R, 4, 128), f32),
            pltpu.VMEM((3, ROWS, 512), bf16),
            pltpu.VMEM((R, 3, 4, 128), f32),
            pltpu.VMEM((4, ROWS, 512), bf16),
            pltpu.VMEM((2, ROWS, 256), bf16),
            pltpu.VMEM((2, ROWS, 256), bf16),
            pltpu.VMEM((2, ROWS, 512), bf16),
            pltpu.VMEM((PARTS[-1][1], 512), bf16),
            dma((6,)),
            dma((len(set(KEY_SEM.values())),)),
            dma((3, 2)),
            dma((3,)),
            dma((R,)),
            dma((R,)),
            dma((R, 3)),
            dma((8,)),
        ],
        compiler_params=pltpu.CompilerParams(
            collective_id=0, has_side_effects=True, vmem_limit_bytes=48 * 2**20
        ),
    )(*(
        pltpu.with_memory_space_constraint(a, pltpu.HBM)
        for a in (span_ids, query_nope, query_rope, cache.T, key_up, value_up, out_proj)
    ))


def solution(mesh):
    rows = ("outer", "inner")
    return jax.shard_map(
        shards,
        mesh=mesh,
        in_specs=(
            P(rows, "head"),
            P(rows, "head"),
            P(rows, None),
            P(rows),
            P(None, "head"),
            P(None, "head"),
            P("head", None),
        ),
        out_specs=P(rows, "head"),
        check_vma=False,
    )
```
